32 devices in a mesh: lat: 4 (over y, x), lon: 4 (over z), lev: 2 (over core).
Axes of the slice: x: 2, y: 2, z: 4, core: 2. Of those that a mesh axis runs over, the one named last changes fastest.
Arguments:
- increment: float32 [80, 64, 512], P('lev', 'lat', 'lon'), may hold values from -6 to 6
- wind_u: float32 [80, 64, 512], P('lev', 'lat', 'lon'), may hold values from -0.4 to 0.4
- wind_v: float32 [80, 64, 512], P('lev', 'lat', 'lon'), may hold values from -0.4 to 0.4
- diffusion: float32 [80], P('lev'), may hold values from 0.02 to 0.2
- mixing: float32 [80, 80], P('lev'), may hold values from -0.15625 to 0.15625
- jacobian: bfloat16 [128, 80], P(None, 'lev'), may hold values from -0.625 to 0.625
- obs_weight: float32 [128], replicated, may hold values from 0.5 to 4
- innovation: bfloat16 [2, 4, 4, 16, 128, 128], P(None, 'lat', 'lon'), may hold values from -6 to 6
- counts: int32 [4, 4], P('lat', 'lon'), may hold values from 1 to 16, as said below
- column_lookup: int32 [4, 4, 2048], P('lat', 'lon'), may hold values from 0 to 2047, each once within a row
Outputs:
- gradient: float32 [80, 64, 512], P('lev', 'lat', 'lon')
- cost: float32 [], replicated
The draws below stay inside these ranges and needn't reach their ends.
Inputs may be any that keep to these rules, and one draw needn't show every extreme that they name: In every row of tiles with one latitude index the counts sum to 24, and the largest of them is 16.
All inputs are finite; a program needn't handle non-finite values.
Results may differ from the reference program's by a relative error of at most 0.005.
Values may be sent and summed in bfloat16 or wider, within the bound.
No kernel may reach another device: no remote copies, remote signals or barrier semaphores. Data moves between devices by JAX's collectives and lax.ppermute only.
A program may use at most 64 MiB of HBM per device.

```python
import math
import jax
import jax.numpy as jnp
from jax import lax

MODEL_LEVELS = 80
CHANNEL_TOTAL = 128
WINDOW_STEPS = 2
BLOCK_COLUMNS = 128
CLON = 128
CLAT = 16
SLOTS_PER_TILE = 16
MEAN_LIVE_BLOCKS = 6
LATITUDE_TILES = 4
LONGITUDE_TILES = 4
NLAT = 64
NLON = 512


def draw_counts(key, part):
    folded = jax.random.fold_in(key, 7331)
    key_swath, key_extra = jax.random.split(folded, 2)
    swath = jax.random.randint(key_swath, (LATITUDE_TILES,), 0, LONGITUDE_TILES)
    place = jnp.arange(LONGITUDE_TILES, dtype=jnp.int32)[None, :]
    swath_flag = place == swath[:, None]
    remaining_slots = MEAN_LIVE_BLOCKS * LONGITUDE_TILES - SLOTS_PER_TILE
    tile_portion = remaining_slots // (LONGITUDE_TILES - 1)
    leftover = remaining_slots - tile_portion * (LONGITUDE_TILES - 1)
    scores = jax.random.randint(key_extra, (LATITUDE_TILES, LONGITUDE_TILES), 0, 1 << 20) * LONGITUDE_TILES + place
    scores = jnp.where(swath_flag, -1, scores)
    order = jnp.argsort(-scores, axis=1)
    ranks = jnp.argsort(order, axis=1)
    surplus_blocks = (ranks < leftover).astype(jnp.int32)
    return jnp.where(swath_flag, SLOTS_PER_TILE, tile_portion + surplus_blocks).astype(jnp.int32)


def steps_of(own_key, extent, pieces, low, high):
    level, own = 1.0, jax.random.fold_in(own_key, 6)
    for position, parts in pieces:
        steps = jnp.exp(jax.random.uniform(jax.random.fold_in(own, position), (parts,), jnp.float32, low / len(pieces), high / len(pieces)))
        level = level * jnp.repeat(steps, extent[position] // parts).reshape([-1 if axis == position else 1 for axis in range(len(extent))])
    return level


def bell_draw(stream_key, shape, deviation, limit, shards=(), held_as=jnp.bfloat16):
    factor_of = steps_of(stream_key, shape, shards, -0.22, 0.18) if shards else 1.0
    values = jax.random.normal(stream_key, shape, jnp.float32) * deviation * factor_of
    return jnp.minimum(jnp.maximum(values, -limit), limit).astype(held_as)


def setup_inputs(seed: int = 0) -> dict:
    streams_of = jax.random.split(jax.random.key(seed), 11)
    return {
        "increment": bell_draw(streams_of[0], (MODEL_LEVELS, NLAT, NLON), 1.0, 6.0, ((0, 2), (1, 4), (2, 4)), jnp.float32),
        "wind_u": jnp.clip(jax.random.uniform(streams_of[1], (MODEL_LEVELS, NLAT, NLON), jnp.float32, -0.4, 0.4) * steps_of(streams_of[1], (MODEL_LEVELS, NLAT, NLON), ((0, 2), (1, 4), (2, 4)), -0.4, 0.0), -0.4, 0.4),
        "wind_v": jnp.clip(jax.random.uniform(streams_of[2], (MODEL_LEVELS, NLAT, NLON), jnp.float32, -0.4, 0.4) * steps_of(streams_of[2], (MODEL_LEVELS, NLAT, NLON), ((0, 2), (1, 4), (2, 4)), -0.4, 0.0), -0.4, 0.4),
        "diffusion": jnp.clip(jnp.exp(math.log(0.2) - 2.3025851 * jax.random.uniform(streams_of[3], (MODEL_LEVELS,), jnp.float32) ** steps_of(streams_of[3], (MODEL_LEVELS,), ((0, 2),), -0.2, 0.2)), 0.02, 0.2),
        "mixing": bell_draw(streams_of[4], (MODEL_LEVELS, MODEL_LEVELS), (16 * MODEL_LEVELS) ** -0.5, 0.15625, ((0, 2),), jnp.float32),
        "jacobian": bell_draw(streams_of[5], (CHANNEL_TOTAL, MODEL_LEVELS), MODEL_LEVELS ** -0.5, 0.625, ((1, 2),)),
        "obs_weight": jnp.clip(jnp.exp(jax.random.uniform(streams_of[6], (CHANNEL_TOTAL,), jnp.float32, math.log(0.5), math.log(4.0))), 0.5, 4.0),
        "innovation": bell_draw(streams_of[7], (WINDOW_STEPS, LATITUDE_TILES, LONGITUDE_TILES, SLOTS_PER_TILE, CHANNEL_TOTAL, BLOCK_COLUMNS), 1.0, 6.0, ((1, 4), (2, 4))),
        "counts": draw_counts(jax.random.fold_in(streams_of[10], 71), 0),
        "column_lookup": jax.vmap(lambda own: jax.random.permutation(own, SLOTS_PER_TILE * BLOCK_COLUMNS))(jax.random.split(streams_of[9], LATITUDE_TILES * LONGITUDE_TILES)).reshape((LATITUDE_TILES, LONGITUDE_TILES, SLOTS_PER_TILE * BLOCK_COLUMNS)).astype(jnp.int32),
    }


def horizontal(field, diffusion, wind_u, wind_v):
    lat_pad = jnp.pad(field, ((0, 0), (1, 1), (0, 0)))
    northern = lat_pad[:, 2:, :]
    southern = lat_pad[:, :-2, :]
    eastern = jnp.roll(field, -1, axis=2)
    western = jnp.roll(field, 1, axis=2)
    coefficient = diffusion[:, None, None]
    result = field + coefficient * (northern + southern + eastern + western - 4.0 * field)
    return result - 0.5 * wind_u * (eastern - western) - 0.5 * wind_v * (northern - southern)

def vertical(smooth, mixing):
    flat = smooth.reshape(MODEL_LEVELS, -1)
    mixed = jnp.dot(mixing, flat, precision=lax.Precision.HIGHEST, preferred_element_type=jnp.float32)
    return smooth + mixed.reshape(smooth.shape)

def to_tiles(field):
    shaped = field.reshape(MODEL_LEVELS, LATITUDE_TILES, CLAT, LONGITUDE_TILES, CLON).transpose(1, 3, 0, 2, 4)
    return shaped.reshape(LATITUDE_TILES, LONGITUDE_TILES, MODEL_LEVELS, CLAT * CLON)

def from_tiles(tiled):
    shaped = tiled.reshape(LATITUDE_TILES, LONGITUDE_TILES, MODEL_LEVELS, CLAT, CLON).transpose(2, 0, 3, 1, 4)
    return shaped.reshape(MODEL_LEVELS, NLAT, NLON)

def pick_columns(tiled, table):
    return jax.vmap(jax.vmap(lambda field, index: jnp.take(field, index, axis=1)))(tiled, table)

def reference(increment, wind_u, wind_v, diffusion, mixing, jacobian, obs_weight, innovation, counts, column_lookup):
    jac_wide = jacobian.astype(jnp.float32)
    active_blocks = (jnp.arange(SLOTS_PER_TILE)[None, None, :] < counts[:, :, None]).astype(jnp.float32)
    inverse = jnp.argsort(column_lookup, axis=2).astype(jnp.int32)
    state = increment
    forcings = []
    misfit_total = jnp.zeros((), jnp.float32)
    for step in range(WINDOW_STEPS):
        state = vertical(horizontal(state, diffusion, wind_u, wind_v), mixing)
        selected_columns = pick_columns(to_tiles(state), column_lookup)
        column_profile = selected_columns.astype(jnp.bfloat16).reshape(LATITUDE_TILES, LONGITUDE_TILES, MODEL_LEVELS, SLOTS_PER_TILE, BLOCK_COLUMNS)
        column_profile = lax.optimization_barrier(column_profile).astype(jnp.float32)
        evolved = jnp.einsum('nl,ijlsc->ijsnc', jac_wide, column_profile, precision=lax.Precision.HIGHEST)
        misfit = active_blocks[..., None, None] * (evolved - innovation[step].astype(jnp.float32))
        scaled = obs_weight[:, None] * misfit
        misfit_total = misfit_total + jnp.sum(misfit * scaled)
        scaled_half = lax.optimization_barrier(scaled.astype(jnp.bfloat16)).astype(jnp.float32)
        return_path = jnp.einsum('nl,ijsnc->ijlsc', jac_wide, scaled_half, precision=lax.Precision.HIGHEST)
        return_path = return_path.astype(jnp.bfloat16)
        dispersed_blocks = lax.optimization_barrier(return_path).astype(jnp.float32).reshape(LATITUDE_TILES, LONGITUDE_TILES, MODEL_LEVELS, SLOTS_PER_TILE * BLOCK_COLUMNS)
        forcings.append(from_tiles(pick_columns(dispersed_blocks, inverse)))
    zero_field = jnp.zeros_like(increment)
    adjoint = zero_field
    for step in range(WINDOW_STEPS - 1, -1, -1):
        adjoint = adjoint + forcings[step]
        coupled = adjoint + jnp.dot(mixing.T, adjoint.reshape(MODEL_LEVELS, -1), precision=lax.Precision.HIGHEST, preferred_element_type=jnp.float32).reshape(adjoint.shape)
        pullback = jax.vjp(lambda field: horizontal(field, diffusion, wind_u, wind_v), zero_field)[1]
        adjoint = pullback(coupled)[0]
    gradient = increment + adjoint
    cost = (0.5 * jnp.sum(increment * increment) + 0.5 * misfit_total) / (MODEL_LEVELS * NLAT * NLON)
    return (gradient, cost)
```

```python
import functools

import jax
import jax.numpy as jnp
from jax import lax
from jax.experimental import pallas as pl
from jax.experimental.pallas import tpu as pltpu
from jax.sharding import PartitionSpec as P

B = 128
HALO = 2
GROUP = 4


def roll(x, shift):
    shift %= B
    return x if shift == 0 else pltpu.roll(x, shift, 1)


def lanes_of(level_count):
    return lax.broadcasted_iota(jnp.int32, (level_count, B), 1)


def block(ref, p):
    return ref[:, p * B : (p + 1) * B]


def pack_edges(fields, rows):
    packed = None
    for f, field in enumerate(fields):
        for q in range(rows):
            rolled = roll(field(q + 1), (f * rows + q) * GROUP + 2)
            if packed is None:
                lane = lanes_of(rolled.shape[0])
                packed = jnp.zeros_like(rolled)
            packed = jnp.where(lane // GROUP == f * rows + q, rolled, packed)
    return packed


def side_block(west, own, east, f, rows):
    lane = lanes_of(own.shape[0])
    first = lane % GROUP < 2
    low, high = -f * rows * GROUP, B // 2 - f * rows * GROUP
    western = jnp.where(first, roll(west, low), roll(own, low))
    eastern = jnp.where(first, roll(own, high), roll(east, high))
    return jnp.where(lane < B // 2, western, eastern)


def from_east(x, side, q):
    lane = lanes_of(x.shape[0])
    return jnp.where(lane == B - 1, roll(side, B - 1 - (B // 2 + q * GROUP + 2)), roll(x, -1))


def from_west(x, side, q):
    lane = lanes_of(x.shape[0])
    return jnp.where(lane == 0, roll(side, -(q * GROUP + 1)), roll(x, 1))


def put_split(stack, p, x):
    levels = x.shape[0]
    head = x.astype(jnp.bfloat16)
    stack[0:levels, p * B : (p + 1) * B] = head
    stack[levels : 2 * levels, p * B : (p + 1) * B] = head
    stack[2 * levels : 3 * levels, p * B : (p + 1) * B] = (x - head.astype(jnp.float32)).astype(jnp.bfloat16)


def clear_rest(stack, levels):
    if stack.shape[0] > 3 * levels:
        stack[3 * levels :, :] = jnp.zeros((stack.shape[0] - 3 * levels, stack.shape[1]), stack.dtype)


def split_matrix(matrix, levels):
    lane = lanes_of(levels)
    matrix = jnp.where(lane < levels, matrix, 0.0)
    head = matrix.astype(jnp.bfloat16).astype(jnp.float32)
    rest = matrix - head
    over = B - levels
    low = jnp.where(lane < levels, head, roll(rest, levels))
    high = jnp.where(lane < levels - over, roll(rest, -over), roll(head, levels - over))
    high = jnp.where(lane < 2 * levels - over, high, 0.0)
    return jnp.concatenate([low, high], axis=1).astype(jnp.bfloat16)


def arrange(rows, place, inc, u, v, inc2, u2, v2, own_par, other_par, main_i, main_u, main_v, inner, edge, par):
    core = place[0]
    levels, half = own_par.shape[0], rows // 2
    own = pl.multiple_of(core * levels, 8)
    other = pl.multiple_of((1 - core) * levels, 8)
    par[pl.ds(own, levels), :] = own_par[...]
    par[pl.ds(other, levels), :] = other_par[...]
    for f, (a, b, main) in enumerate(((inc, inc2, main_i), (u, u2, main_u), (v, v2, main_v))):
        for src, dst in ((a, own), (b, other)):
            for j in range(half):
                main[pl.ds(dst, levels), j * B : (j + 1) * B] = src[pl.ds(core * half + j, levels, stride=rows), :]
            for j in range(HALO):
                k = f * HALO + j
                inner[pl.ds(dst, levels), k * B : (k + 1) * B] = src[
                    pl.ds(half - core * HALO + j, levels, stride=rows), :
                ]
                edge[pl.ds(dst, levels), k * B : (k + 1) * B] = src[
                    pl.ds(core * (rows - HALO) + j, levels, stride=rows), :
                ]


def by_column(place, lookup, observed, out, live, hot, stacked):
    core, count = place[0], place[3]
    steps, slots, channels, width = observed.shape
    columns = hot.shape[0]
    index = lax.broadcasted_iota(jnp.int32, (columns, width), 0)
    for s in range(slots):
        target = jnp.where(s < count, lookup[s : s + 1, :] - core * columns, -1)
        hot[:, s * width : (s + 1) * width] = jnp.where(index == target, 1.0, 0.0).astype(jnp.bfloat16)
        for t in range(steps):
            stacked[t * channels : (t + 1) * channels, s * width : (s + 1) * width] = observed[t, s]
    tail = stacked.shape[0] - steps * channels
    stacked[steps * channels :, :] = jnp.ones((tail, slots * width), jnp.bfloat16)
    moved = lax.dot_general(
        stacked[...], hot[...], (((1,), (1,)), ((), ())), preferred_element_type=jnp.float32
    )
    out[...] = moved[: steps * channels].astype(jnp.bfloat16)
    live[...] = moved[steps * channels : steps * channels + 8]


def windows(place, main_i, main_u, main_v, inner, edge, win_i, win_u, win_v, packed):
    low = place[0] == 0
    count = win_i.shape[1] // B
    for f, (main, win) in enumerate(((main_i, win_i), (main_u, win_u), (main_v, win_v))):
        win[:, HALO * B : (count - HALO) * B] = main[...]
        span = slice(f * HALO * B, (f + 1) * HALO * B)
        near, far = inner[:, span], edge[:, span]
        win[:, : HALO * B] = jnp.where(low, far, near)
        win[:, (count - HALO) * B :] = jnp.where(low, near, far)
    packed[...] = pack_edges([functools.partial(block, win) for win in (win_i, win_u, win_v)], count - 2)


def smooth(x, north, south, east, west, diff, u, v):
    return (
        x
        + diff * ((north + south) + (east + west) - 4.0 * x)
        - 0.5 * u * (east - west)
        - 0.5 * v * (north - south)
    )


def forward(
    place, win_i, win_u, win_v, west, own, east, par, weight, observed, live,
    f1, f2, edge, inner, cost, stack, plain, state,
):
    levels = par.shape[0]
    count = win_i.shape[1] // B
    rows = count - 2
    half = rows - 2
    diff = par[:, levels : levels + 1]
    coupling = split_matrix(par[:, :B], levels)
    radiance = par[:, B:].astype(jnp.bfloat16)
    channels = radiance.shape[1]
    diagonal = lax.broadcasted_iota(jnp.int32, (channels, channels), 0) == lax.broadcasted_iota(
        jnp.int32, (channels, channels), 1
    )
    weights = jnp.sum(jnp.where(diagonal, weight[...], 0.0), axis=1, keepdims=True)
    clear_rest(stack, levels)
    sides = [side_block(west[...], own[...], east[...], f, rows) for f in range(3)]
    for q in range(rows):
        p = q + 1
        x = block(win_i, p)
        s = smooth(
            x, block(win_i, p + 1), block(win_i, p - 1), from_east(x, sides[0], q), from_west(x, sides[0], q),
            diff, block(win_u, p), block(win_v, p),
        )
        plain[:, q * B : (q + 1) * B] = s
        put_split(stack, q, s)
    x = sides[0]
    s = smooth(x, roll(x, -GROUP), roll(x, GROUP), roll(x, -1), roll(x, 1), diff, sides[1], sides[2])
    plain[:, rows * B :] = s
    put_split(stack, rows, s)
    state[...] = plain[...] + jnp.dot(coupling, stack[...], preferred_element_type=jnp.float32)
    first, final = (rows - 1) * B, rows * B
    state[:, :B] = jnp.where(place[1] == 1, state[:, :B], 0.0)
    state[:, first:final] = jnp.where(place[2] == 1, state[:, first:final], 0.0)

    def observe(profile, t, out):
        evolved = lax.dot_general(
            radiance, profile, (((0,), (0,)), ((), ())), preferred_element_type=jnp.float32
        )
        departure = evolved - observed[t * channels : (t + 1) * channels, :].astype(jnp.float32)
        misfit = live[0:1, :] * departure
        scaled = weights * misfit
        back = jnp.dot(radiance, scaled.astype(jnp.bfloat16), preferred_element_type=jnp.float32)
        out[...] = back.astype(jnp.bfloat16)
        return jnp.sum(misfit * scaled, keepdims=True)

    total = observe(state[:, B : (half + 1) * B].astype(jnp.bfloat16), 0, f1)
    side = state[:, rows * B :]
    for q in range(1, rows - 1):
        x = block(state, q)
        s = smooth(
            x, block(state, q + 1), block(state, q - 1), from_east(x, side, q), from_west(x, side, q),
            diff, block(win_u, q + 1), block(win_v, q + 1),
        )
        plain[:, (q - 1) * B : q * B] = s
        put_split(stack, q - 1, s)
    end = plain[:, : half * B] + jnp.dot(coupling, stack[:, : half * B], preferred_element_type=jnp.float32)
    total = total + observe(end.astype(jnp.bfloat16), 1, f2)
    whole = win_i[:, HALO * B : (count - HALO) * B]
    total = 0.5 * (total + jnp.sum(whole * whole, keepdims=True))
    cost[...] = jnp.broadcast_to(total, cost.shape)
    low = place[0] == 0
    span = HALO * B
    for k, f in enumerate((f2, f1)):
        head, tail = f[:, :span].astype(jnp.float32), f[:, (half - HALO) * B :].astype(jnp.float32)
        edge[:, k * span : (k + 1) * span] = jnp.where(low, head, tail).astype(jnp.bfloat16)
        inner[:, k * span : (k + 1) * span] = jnp.where(low, tail, head).astype(jnp.bfloat16)


def forcing_windows(place, f1, f2, edge, inner, cost, other_cost, win_1, win_2, packed):
    low = place[0] == 0
    count = win_1.shape[1] // B
    span = HALO * B
    for k, (f, win) in enumerate(((f2, win_2), (f1, win_1))):
        win[:, span : (count - HALO) * B] = f[...].astype(jnp.float32)
        far = edge[:, k * span : (k + 1) * span].astype(jnp.float32)
        near = inner[:, k * span : (k + 1) * span].astype(jnp.float32)
        win[:, :span] = jnp.where(low, far, near)
        win[:, (count - HALO) * B :] = jnp.where(low, near, far)
    both = pack_edges([functools.partial(block, win) for win in (win_2, win_1)], count - 2)
    total = cost[0:1, :] + other_cost[0:1, :]
    packed[...] = jnp.where(lanes_of(both.shape[0]) == B - 1, total, both)


def backward(
    place, win_1, win_2, fwest, fown, feast, win_i, win_u, win_v, west, own, east, par,
    kept, sent, stack, coupled, square,
):
    levels = par.shape[0]
    count = win_i.shape[1] // B
    rows = count - 2
    half = rows - 2
    diff = par[:, levels : levels + 1]
    middle = 1.0 - 4.0 * diff
    square[...] = jnp.zeros(square.shape, jnp.float32)
    square[:levels, :] = jnp.where(lanes_of(levels) < levels, par[:, :B], 0.0)
    coupling = split_matrix(jnp.transpose(square[...])[:levels], levels)
    clear_rest(stack, levels)
    f_sides = [side_block(fwest[...], fown[...], feast[...], f, rows) for f in range(2)]
    sides = [side_block(west[...], own[...], east[...], f, rows) for f in range(3)]
    for p in range(count):
        x = block(win_2, p)
        coupled[:, p * B : (p + 1) * B] = x
        put_split(stack, p, x)
    coupled[:, count * B :] = f_sides[0]
    put_split(stack, count, f_sides[0])
    coupled[...] = coupled[...] + jnp.dot(coupling, stack[...], preferred_element_type=jnp.float32)

    def spread(p, q, side):
        x = block(coupled, p)
        north = (diff + 0.5 * block(win_v, q + 2)) * block(coupled, p + 1)
        south = (diff - 0.5 * block(win_v, q)) * block(coupled, p - 1)
        u = 0.5 * block(win_u, q + 1)
        side_east = (diff + 0.5 * sides[1]) * side
        side_west = (diff - 0.5 * sides[1]) * side
        return (
            middle * x + north + south + from_east((diff + u) * x, side_east, q)
            + from_west((diff - u) * x, side_west, q)
        )

    side = coupled[:, count * B :]
    after = []
    side_v, side_u = 0.5 * sides[2], 0.5 * sides[1]
    result = (
        middle * side
        + roll((diff + side_v) * side, -GROUP)
        + roll((diff - side_v) * side, GROUP)
        + roll((diff + side_u) * side, -1)
        + roll((diff - side_u) * side, 1)
        + f_sides[1]
    )
    for q in range(rows):
        after.append(spread(q + 1, q, side) + block(win_1, q + 1))
    after[0] = jnp.where(place[1] == 1, after[0], 0.0)
    after[-1] = jnp.where(place[2] == 1, after[-1], 0.0)
    for q in range(rows):
        coupled[:, (q + 1) * B : (q + 2) * B] = after[q]
        put_split(stack, q, after[q])
    coupled[:, count * B :] = result
    put_split(stack, rows, result)
    mixed = jnp.dot(coupling, stack[:, : (rows + 1) * B], preferred_element_type=jnp.float32)
    coupled[:, B : (rows + 1) * B] = coupled[:, B : (rows + 1) * B] + mixed[:, : rows * B]
    side = coupled[:, count * B :] + mixed[:, rows * B :]
    low = place[0] == 0
    part = levels // 2
    for j in range(half):
        value = block(win_i, j + HALO) + spread(j + HALO, j + 1, side)
        kept[pl.ds(j, part, stride=half), :] = jnp.where(low, value[:part], value[part:])
        sent[pl.ds(j, part, stride=half), :] = jnp.where(low, value[part:], value[:part])


def call(kernel, outs, scratch=(), name=None):
    vmem = pl.BlockSpec(memory_space=pltpu.VMEM)

    def run(place, *operands):
        return pl.pallas_call(
            kernel,
            out_shape=[jax.ShapeDtypeStruct(shape, dtype) for shape, dtype in outs],
            in_specs=[pl.BlockSpec(memory_space=pltpu.SMEM)] + [vmem] * len(operands),
            out_specs=[vmem] * len(outs),
            scratch_shapes=[pltpu.VMEM(shape, dtype) for shape, dtype in scratch],
            name=name,
        )(place, *operands)

    return run


def ring(x, axis, shift):
    count = lax.axis_size(axis)
    return lax.ppermute(x, axis, [(i, (i + shift) % count) for i in range(count)])


def body(
    increment, wind_u, wind_v, diffusion, mixing, jacobian, obs_weight, innovation, counts, column_lookup
):
    part, rows, width = increment.shape
    levels = mixing.shape[1]
    steps, channels = innovation.shape[0], innovation.shape[-2]
    slots = innovation.shape[3]
    assert width == B and steps == HALO and levels == 2 * part
    half = rows // 2
    count = half + 2 * HALO
    columns = half * B
    f32, bf16 = jnp.float32, jnp.bfloat16
    core, lat = lax.axis_index("lev"), lax.axis_index("lat")
    tiles = lax.axis_size("lat")
    at_top = (core == 0) & (lat == 0)
    at_end = (core == 1) & (lat == tiles - 1)
    place = jnp.stack(
        [core.astype(jnp.int32), 1 - at_top.astype(jnp.int32), 1 - at_end.astype(jnp.int32), counts[0, 0]]
    )
    pairs = [(2 * i + 1, 2 * i + 2) for i in range(tiles - 1)]
    pairs = pairs + [(b, a) for a, b in pairs]

    def swap(x):
        return lax.ppermute(x, "lev", [(0, 1), (1, 0)])

    def across(x):
        return lax.ppermute(x, ("lat", "lev"), pairs)

    own_par = jnp.concatenate(
        [
            mixing,
            diffusion[:, None],
            jnp.zeros((part, B - levels - 1), f32),
            jacobian.T.astype(f32),
        ],
        axis=1,
    )
    fields = [x.reshape(part * rows, B) for x in (increment, wind_u, wind_v)]
    others = [swap(x) for x in fields]
    other_par = swap(own_par)
    main = ((levels, columns), f32)
    edges = ((levels, 3 * HALO * B), f32)
    win = ((levels, count * B), f32)
    packed = ((levels, B), f32)
    *mains, inner, edge, par = call(
        functools.partial(arrange, rows), [main] * 3 + [edges] * 2 + [((levels, 2 * B), f32)], name="arrange"
    )(place, *fields, *others, own_par, other_par)
    edge = across(edge)
    observed, live = call(
        by_column,
        [((steps * channels, columns), bf16), ((8, columns), f32)],
        [((columns, slots * B), bf16), ((steps * channels + 16, slots * B), bf16)],
        name="by_column",
    )(place, column_lookup.reshape(slots, B), innovation.reshape(steps, slots, channels, B))
    win_i, win_u, win_v, own = call(windows, [win] * 3 + [packed], name="windows")(place, *mains, inner, edge)
    west, east = ring(own, "lon", 1), ring(own, "lon", -1)
    forcing = ((levels, columns), bf16)
    f_edges = ((levels, 2 * HALO * B), bf16)
    depth = -(-3 * levels // 16) * 16
    depth = max(depth, 2 * B)
    f1, f2, f_edge, f_inner, cost = call(
        forward,
        [forcing] * 2 + [f_edges] * 2 + [((8, B), f32)],
        [((depth, (count - 1) * B), bf16), ((levels, (count - 1) * B), f32), ((levels, (count - 1) * B), f32)],
        name="forward",
    )(place, win_i, win_u, win_v, west, own, east, par, obs_weight.reshape(1, -1), observed, live)
    f_edge, f_inner = across(f_edge), swap(f_inner)
    cost_2 = ring(cost, "lat", 1)
    win_1, win_2, f_own = call(forcing_windows, [win] * 2 + [packed], name="forcing")(
        place, f1, f2, f_edge, f_inner, cost, cost_2
    )
    f_west, f_east = ring(f_own, "lon", 1), ring(f_own, "lon", -1)
    total = f_own[:8] + f_west[:8]
    shift = 2
    while shift < tiles:
        total = total + ring(total, "lat", shift)
        shift *= 2
    kept, sent = call(
        backward,
        [((part * half, B), f32)] * 2,
        [((depth, (count + 1) * B), bf16), ((levels, (count + 1) * B), f32), ((B, B), f32)],
        name="backward",
    )(place, win_1, win_2, f_west, f_own, f_east, win_i, win_u, win_v, west, own, east, par)
    got = swap(sent)
    shift = 2
    while shift < lax.axis_size("lon"):
        total = total + ring(total, "lon", shift)
        shift *= 2
    total = total + swap(total)
    kept, got = kept.reshape(part, half, B), got.reshape(part, half, B)
    gradient = jnp.where(
        core == 0, jnp.concatenate([kept, got], axis=1), jnp.concatenate([got, kept], axis=1)
    )
    cells = increment.size * tiles * lax.axis_size("lon") * lax.axis_size("lev")
    return gradient, total[0, B - 1] / cells


def solution(mesh):
    for axis in ("lat", "lon"):
        assert mesh.shape[axis] & (mesh.shape[axis] - 1) == 0 and mesh.shape[axis] > 1
    in_specs = (
        P("lev", "lat", "lon"),
        P("lev", "lat", "lon"),
        P("lev", "lat", "lon"),
        P("lev"),
        P("lev", None),
        P(None, "lev"),
        P(),
        P(None, "lat", "lon", None, None, None),
        P("lat", "lon"),
        P("lat", "lon", None),
    )
    out_specs = (P("lev", "lat", "lon"), P())
    return jax.shard_map(body, mesh=mesh, in_specs=in_specs, out_specs=out_specs, check_vma=False)
```

```python
import functools

import jax
import jax.numpy as jnp
from jax import lax
from jax.experimental import pallas as pl
from jax.experimental.pallas import tpu as pltpu
from jax.sharding import PartitionSpec as P

B = 128
HALO = 2
GROUP = 4


def roll(x, shift):
    shift %= B
    return x if shift == 0 else pltpu.roll(x, shift, 1)


def lanes_of(level_count):
    return lax.broadcasted_iota(jnp.int32, (level_count, B), 1)


def block(ref, p):
    return ref[:, p * B : (p + 1) * B]


def pack_edges(fields, rows):
    packed = None
    for f, field in enumerate(fields):
        for q in range(rows):
            rolled = roll(field(q + 1), (f * rows + q) * GROUP + 2)
            if packed is None:
                lane = lanes_of(rolled.shape[0])
                packed = jnp.zeros_like(rolled)
            packed = jnp.where(lane // GROUP == f * rows + q, rolled, packed)
    return packed


def side_block(west, own, east, f, rows):
    lane = lanes_of(own.shape[0])
    first = lane % GROUP < 2
    low, high = -f * rows * GROUP, B // 2 - f * rows * GROUP
    western = jnp.where(first, roll(west, low), roll(own, low))
    eastern = jnp.where(first, roll(own, high), roll(east, high))
    return jnp.where(lane < B // 2, western, eastern)


def from_east(x, side, q):
    lane = lanes_of(x.shape[0])
    return jnp.where(lane == B - 1, roll(side, B - 1 - (B // 2 + q * GROUP + 2)), roll(x, -1))


def from_west(x, side, q):
    lane = lanes_of(x.shape[0])
    return jnp.where(lane == 0, roll(side, -(q * GROUP + 1)), roll(x, 1))


def put_split(stack, p, x):
    levels = x.shape[0]
    head = x.astype(jnp.bfloat16)
    stack[0:levels, p * B : (p + 1) * B] = head
    stack[levels : 2 * levels, p * B : (p + 1) * B] = head
    stack[2 * levels : 3 * levels, p * B : (p + 1) * B] = (x - head.astype(jnp.float32)).astype(jnp.bfloat16)


def clear_rest(stack, levels):
    if stack.shape[0] > 3 * levels:
        stack[3 * levels :, :] = jnp.zeros((stack.shape[0] - 3 * levels, stack.shape[1]), stack.dtype)


def split_matrix(matrix, levels):
    lane = lanes_of(levels)
    matrix = jnp.where(lane < levels, matrix, 0.0)
    head = matrix.astype(jnp.bfloat16).astype(jnp.float32)
    rest = matrix - head
    over = B - levels
    low = jnp.where(lane < levels, head, roll(rest, levels))
    high = jnp.where(lane < levels - over, roll(rest, -over), roll(head, levels - over))
    high = jnp.where(lane < 2 * levels - over, high, 0.0)
    return jnp.concatenate([low, high], axis=1).astype(jnp.bfloat16)


def spread_rows(rows, core, sources, level, mains, inner, edge):
    levels = sources[0].shape[0] // rows
    half = rows // 2
    at = pl.ds(level, levels)
    k = 0
    for src, main, width in zip(sources, mains, (HALO, 1, HALO)):
        for j in range(half):
            main[at, j * B : (j + 1) * B] = src[pl.ds(core * half + j, levels, stride=rows), :]
        for j in range(width):
            near = jnp.where(core == 0, half + j, half - width + j)
            far = jnp.where(core == 0, j, rows - width + j)
            lanes = slice(k * B, (k + 1) * B)
            inner[at, lanes] = src[pl.ds(near, levels, stride=rows), :]
            edge[at, lanes] = src[pl.ds(far, levels, stride=rows), :].astype(edge.dtype)
            k += 1


def arrange_own(
    rows, counts, mixing, diffusion, radiance, inc, u, v, main_i, main_u, main_v, inner, edge, par,
    mixing_at, diffusion_at, radiance_at, inc_at, u_at, v_at, arrived,
):
    core = lax.axis_index("lev")
    here = (inc_at, u_at, v_at, mixing_at, diffusion_at, radiance_at)
    copies = [
        pltpu.make_async_copy(src, dst, arrived.at[i])
        for i, (src, dst) in enumerate(zip((inc, u, v, mixing, diffusion, radiance), here))
    ]
    for copy in copies:
        copy.start()
    for copy in copies[3:]:
        copy.wait()
    part, levels = mixing.shape
    square = lax.broadcasted_iota(jnp.int32, (part, part), 0) == lax.broadcasted_iota(jnp.int32, (part, part), 1)
    column = jnp.sum(jnp.where(square, diffusion_at[...], 0.0), axis=1, keepdims=True)
    par[:, :B] = jnp.broadcast_to(column, (part, B))
    par[:, :levels] = mixing_at[...]
    par[:, B:] = radiance_at[...].astype(jnp.float32)
    for copy in copies[:3]:
        copy.wait()
    level = pl.multiple_of(core * part, 8)
    spread_rows(rows, core, (inc_at, u_at, v_at), level, (main_i, main_u, main_v), inner, edge)


def arrange_other(
    rows, counts, inc, u, v, main_i0, main_u0, main_v0, inner0, edge0, main_i, main_u, main_v, inner, edge
):
    core = lax.axis_index("lev")
    level = pl.multiple_of((1 - core) * (inc.shape[0] // rows), 8)
    spread_rows(rows, core, (inc, u, v), level, (main_i, main_u, main_v), inner, edge)


def by_column(counts, after, lookup, observed, weight, out, live, weights, hot, stacked):
    core, count = lax.axis_index("lev"), counts[0, 0]
    steps, slots, channels, width = observed.shape
    columns = hot.shape[0]
    diagonal = lax.broadcasted_iota(jnp.int32, (channels, channels), 0) == lax.broadcasted_iota(
        jnp.int32, (channels, channels), 1
    )
    weights[...] = jnp.broadcast_to(
        jnp.sum(jnp.where(diagonal, weight[...], 0.0), axis=1, keepdims=True), weights.shape
    )
    index = lax.broadcasted_iota(jnp.int32, (columns, width), 0)
    for s in range(slots):
        target = jnp.where(s < count, lookup[s : s + 1, :] - core * columns, -1)
        hot[:, s * width : (s + 1) * width] = jnp.where(index == target, 1.0, 0.0).astype(jnp.bfloat16)
        for t in range(steps):
            stacked[t * channels : (t + 1) * channels, s * width : (s + 1) * width] = observed[t, s]
    tail = stacked.shape[0] - steps * channels
    stacked[steps * channels :, :] = jnp.ones((tail, slots * width), jnp.bfloat16)
    moved = lax.dot_general(
        stacked[...], hot[...], (((1,), (1,)), ((), ())), preferred_element_type=jnp.float32
    )
    out[...] = moved[: steps * channels].astype(jnp.bfloat16)
    live[...] = moved[steps * channels : steps * channels + 8]


def flags():
    core, lat = lax.axis_index("lev"), lax.axis_index("lat")
    first = (core == 1) | (lat > 0)
    final = (core == 0) | (lat < lax.axis_size("lat") - 1)
    return core, first, final


def fill_halo(win, near, far, low, width):
    count = win.shape[1] // B
    win[:, (HALO - width) * B : HALO * B] = jnp.where(low, far, near)
    win[:, (count - HALO) * B : (count - HALO + width) * B] = jnp.where(low, near, far)


def windows(counts, main_i, main_u, main_v, inner, edge, after, win_i, win_u, win_v, packed):
    low = lax.axis_index("lev") == 0
    count = win_i.shape[1] // B
    k = 0
    for main, win, width in ((main_i, win_i, HALO), (main_u, win_u, 1), (main_v, win_v, HALO)):
        win[:, HALO * B : (count - HALO) * B] = main[...]
        span = slice(k * B, (k + width) * B)
        fill_halo(win, inner[:, span], edge[:, span].astype(jnp.float32), low, width)
        k += width
    packed[...] = pack_edges([functools.partial(block, win) for win in (win_i, win_u, win_v)], count - 2)


def smooth(x, north, south, east, west, diff, u, v):
    return (
        x
        + diff * ((north + south) + (east + west) - 4.0 * x)
        - 0.5 * u * (east - west)
        - 0.5 * v * (north - south)
    )


def forward(
    counts, win_i, win_u, win_v, west, own, east, own_par, other_par, observed, live, weights,
    f1, f2, edge, inner, cost, par, stack, plain, state,
):
    core, is_first, is_final = flags()
    part = own_par.shape[0]
    par[pl.ds(pl.multiple_of(core * part, 8), part), :] = own_par[...]
    par[pl.ds(pl.multiple_of((1 - core) * part, 8), part), :] = other_par[...]
    levels = par.shape[0]
    count = win_i.shape[1] // B
    rows = count - 2
    half = rows - 2
    diff = par[:, levels : levels + 1]
    coupling = split_matrix(par[:, :B], levels)
    radiance = par[:, B:].astype(jnp.bfloat16)
    channels = radiance.shape[1]
    scale = weights[:, :1]
    clear_rest(stack, levels)
    sides = [side_block(west[...], own[...], east[...], f, rows) for f in range(3)]
    for q in range(rows):
        p = q + 1
        x = block(win_i, p)
        s = smooth(
            x, block(win_i, p + 1), block(win_i, p - 1), from_east(x, sides[0], q), from_west(x, sides[0], q),
            diff, block(win_u, p), block(win_v, p),
        )
        plain[:, q * B : (q + 1) * B] = s
        put_split(stack, q, s)
    x = sides[0]
    s = smooth(x, roll(x, -GROUP), roll(x, GROUP), roll(x, -1), roll(x, 1), diff, sides[1], sides[2])
    plain[:, rows * B :] = s
    put_split(stack, rows, s)
    state[...] = plain[...] + jnp.dot(coupling, stack[...], preferred_element_type=jnp.float32)
    first, final = (rows - 1) * B, rows * B
    state[:, :B] = jnp.where(is_first, state[:, :B], 0.0)
    state[:, first:final] = jnp.where(is_final, state[:, first:final], 0.0)

    def observe(profile, t, out):
        evolved = lax.dot_general(
            radiance, profile, (((0,), (0,)), ((), ())), preferred_element_type=jnp.float32
        )
        departure = evolved - observed[t * channels : (t + 1) * channels, :].astype(jnp.float32)
        misfit = live[0:1, :] * departure
        scaled = scale * misfit
        back = jnp.dot(radiance, scaled.astype(jnp.bfloat16), preferred_element_type=jnp.float32)
        out[...] = back.astype(jnp.bfloat16)
        return jnp.sum(misfit * scaled, keepdims=True)

    total = observe(state[:, B : (half + 1) * B].astype(jnp.bfloat16), 0, f1)
    side = state[:, rows * B :]
    for q in range(1, rows - 1):
        x = block(state, q)
        s = smooth(
            x, block(state, q + 1), block(state, q - 1), from_east(x, side, q), from_west(x, side, q),
            diff, block(win_u, q + 1), block(win_v, q + 1),
        )
        plain[:, (q - 1) * B : q * B] = s
        put_split(stack, q - 1, s)
    end = plain[:, : half * B] + jnp.dot(coupling, stack[:, : half * B], preferred_element_type=jnp.float32)
    total = total + observe(end.astype(jnp.bfloat16), 1, f2)
    whole = win_i[:, HALO * B : (count - HALO) * B]
    total = 0.5 * (total + jnp.sum(whole * whole, keepdims=True))
    cost[...] = jnp.broadcast_to(total, cost.shape)
    low = core == 0
    k = 0
    for f, width in ((f2, HALO), (f1, 1)):
        head, tail = f[:, : width * B].astype(jnp.float32), f[:, (half - width) * B :].astype(jnp.float32)
        edge[:levels, k * B : (k + width) * B] = jnp.where(low, head, tail).astype(jnp.bfloat16)
        inner[:, k * B : (k + width) * B] = jnp.where(low, tail, head).astype(jnp.bfloat16)
        k += width
    tail = edge.shape[0] - levels
    head = total.astype(jnp.bfloat16).astype(jnp.float32)
    rest = (total - head).astype(jnp.bfloat16).astype(jnp.float32)
    pieces = (head, rest, total - head - rest)
    lane = lanes_of(tail)
    carried = jnp.zeros((tail, B), jnp.float32)
    for i, piece in enumerate(pieces):
        carried = jnp.where(lane == i, piece, carried)
    edge[levels:, :B] = carried.astype(jnp.bfloat16)
    edge[levels:, B:] = jnp.zeros((tail, edge.shape[1] - B), jnp.bfloat16)


def forcing_windows(counts, f1, f2, edge, inner, cost, win_1, win_2, packed, total):
    core, is_first, is_final = flags()
    low = core == 0
    inside = is_first & is_final
    levels = f1.shape[0]
    count = win_1.shape[1] // B
    k = 0
    for f, win, width in ((f2, win_2, HALO), (f1, win_1, 1)):
        win[:, HALO * B : (count - HALO) * B] = f[...].astype(jnp.float32)
        span = slice(k * B, (k + width) * B)
        far = jnp.where(inside, edge[:levels, span].astype(jnp.float32), 0.0)
        fill_halo(win, inner[:, span].astype(jnp.float32), far, low, width)
        k += width
    both = pack_edges([functools.partial(block, win) for win in (win_2, win_1)], count - 2)
    carried = edge[levels:, :B].astype(jnp.float32)
    carried = jnp.sum(jnp.where(lanes_of(carried.shape[0]) < 3, carried, 0.0), axis=1, keepdims=True)
    here = cost[...] + carried[: cost.shape[0]]
    total[...] = here
    packed[...] = jnp.where(lanes_of(both.shape[0]) == B - 1, here[0:1, :], both)


def backward(
    counts, win_1, win_2, fwest, fown, feast, win_i, win_u, win_v, west, own, east, par,
    kept, sent, stack, coupled, square,
):
    core, is_first, is_final = flags()
    levels = par.shape[0]
    count = win_i.shape[1] // B
    rows = count - 2
    half = rows - 2
    diff = par[:, levels : levels + 1]
    middle = 1.0 - 4.0 * diff
    square[...] = jnp.zeros(square.shape, jnp.float32)
    square[:levels, :] = jnp.where(lanes_of(levels) < levels, par[:, :B], 0.0)
    coupling = split_matrix(jnp.transpose(square[...])[:levels], levels)
    clear_rest(stack, levels)
    f_sides = [side_block(fwest[...], fown[...], feast[...], f, rows) for f in range(2)]
    sides = [side_block(west[...], own[...], east[...], f, rows) for f in range(3)]
    for p in range(count):
        x = block(win_2, p)
        coupled[:, p * B : (p + 1) * B] = x
        put_split(stack, p, x)
    coupled[:, count * B :] = f_sides[0]
    put_split(stack, count, f_sides[0])
    coupled[...] = coupled[...] + jnp.dot(coupling, stack[...], preferred_element_type=jnp.float32)

    def spread(p, q, side):
        x = block(coupled, p)
        north = (diff + 0.5 * block(win_v, q + 2)) * block(coupled, p + 1)
        south = (diff - 0.5 * block(win_v, q)) * block(coupled, p - 1)
        u = 0.5 * block(win_u, q + 1)
        side_east = (diff + 0.5 * sides[1]) * side
        side_west = (diff - 0.5 * sides[1]) * side
        return (
            middle * x + north + south + from_east((diff + u) * x, side_east, q)
            + from_west((diff - u) * x, side_west, q)
        )

    side = coupled[:, count * B :]
    after = []
    side_v, side_u = 0.5 * sides[2], 0.5 * sides[1]
    result = (
        middle * side
        + roll((diff + side_v) * side, -GROUP)
        + roll((diff - side_v) * side, GROUP)
        + roll((diff + side_u) * side, -1)
        + roll((diff - side_u) * side, 1)
        + f_sides[1]
    )
    for q in range(rows):
        after.append(spread(q + 1, q, side) + block(win_1, q + 1))
    after[0] = jnp.where(is_first, after[0], 0.0)
    after[-1] = jnp.where(is_final, after[-1], 0.0)
    for q in range(rows):
        coupled[:, (q + 1) * B : (q + 2) * B] = after[q]
        put_split(stack, q, after[q])
    coupled[:, count * B :] = result
    put_split(stack, rows, result)
    mixed = jnp.dot(coupling, stack[:, : (rows + 1) * B], preferred_element_type=jnp.float32)
    coupled[:, B : (rows + 1) * B] = coupled[:, B : (rows + 1) * B] + mixed[:, : rows * B]
    side = coupled[:, count * B :] + mixed[:, rows * B :]
    low = core == 0
    part = levels // 2
    for j in range(half):
        value = block(win_i, j + HALO) + spread(j + HALO, j + 1, side)
        kept[pl.ds(j, part, stride=half), :] = jnp.where(low, value[:part], value[part:])
        sent[pl.ds(j, part, stride=half), :] = jnp.where(low, value[part:], value[:part])


def call(kernel, outs, scratch=(), name=None, aliases=None, in_hbm=False, flops=10**9):
    vmem = pl.BlockSpec(memory_space=pltpu.VMEM)
    source = pl.BlockSpec(memory_space=pltpu.HBM) if in_hbm else vmem

    def run(counts, *operands):
        if in_hbm:
            operands = [pltpu.with_memory_space_constraint(x, pltpu.HBM) for x in operands]
        return pl.pallas_call(
            kernel,
            out_shape=[jax.ShapeDtypeStruct(shape, dtype) for shape, dtype in outs],
            in_specs=[pl.BlockSpec(memory_space=pltpu.SMEM)] + [source] * len(operands),
            out_specs=[vmem] * len(outs),
            scratch_shapes=[
                pltpu.SemaphoreType.DMA(shape) if dtype is None else pltpu.VMEM(shape, dtype)
                for shape, dtype in scratch
            ],
            input_output_aliases=aliases or {},
            name=name,
            cost_estimate=pl.CostEstimate(flops=flops, bytes_accessed=0, transcendentals=0),
            compiler_params=pltpu.CompilerParams(vmem_limit_bytes=24 * 2**20),
        )(counts, *operands)

    return run


def ring(x, axis, shift):
    count = lax.axis_size(axis)
    return lax.ppermute(x, axis, [(i, (i + shift) % count) for i in range(count)])


def body(
    increment, wind_u, wind_v, diffusion, mixing, jacobian, obs_weight, innovation, counts, column_lookup
):
    part, rows, width = increment.shape
    levels = mixing.shape[1]
    steps, channels = innovation.shape[0], innovation.shape[-2]
    slots = innovation.shape[3]
    assert width == B and steps == HALO and levels == 2 * part
    half = rows // 2
    count = half + 2 * HALO
    columns = half * B
    f32, bf16 = jnp.float32, jnp.bfloat16
    tiles, along = lax.axis_size("lat"), lax.axis_size("lon")
    pairs = [(2 * i + 1, (2 * i + 2) % (2 * tiles)) for i in range(tiles)]
    pairs = pairs + [(b, a) for a, b in pairs]
    inside = [(a, b) for a, b in pairs if abs(a - b) == 1]

    def swap(x):
        return lax.ppermute(x, "lev", [(0, 1), (1, 0)])

    def across(x, which):
        return lax.ppermute(x, ("lat", "lev"), which)

    fields = [x.reshape(part * rows, B) for x in (increment, wind_u, wind_v)]
    others = [swap(x) for x in fields]
    halo = 2 * HALO + 1
    main = ((levels, columns), f32)
    groups = [main] * 3 + [((levels, halo * B), f32), ((levels, halo * B), bf16)]
    win = ((levels, count * B), f32)
    packed = ((levels, B), f32)
    field = ((part * rows, B), f32)
    *sorted_rows, own_par = call(
        functools.partial(arrange_own, rows),
        groups + [((part, 2 * B), f32)],
        [((part, levels), f32), ((1, part), f32), ((part, channels), bf16)] + [field] * 3 + [((6,), None)],
        name="arrange_own",
        in_hbm=True,
    )(counts, mixing, diffusion.reshape(1, -1), jacobian.T, *fields)
    *mains, inner, edge = call(
        functools.partial(arrange_other, rows), groups, name="arrange_other",
        aliases={4 + i: i for i in range(5)},
    )(counts, *others, *sorted_rows)
    edge = across(edge, inside)
    other_par = swap(own_par)
    observed, live, weights = call(
        by_column,
        [((steps * channels, columns), bf16), ((8, columns), f32), ((channels, B), f32)],
        [((columns, slots * B), bf16), ((steps * channels + 16, slots * B), bf16)],
        name="by_column",
    )(
        counts, inner, column_lookup.reshape(slots, B), innovation.reshape(steps, slots, channels, B),
        obs_weight.reshape(1, -1),
    )
    win_i, win_u, win_v, own = call(windows, [win] * 3 + [packed], name="windows")(
        counts, *mains, inner, edge, live
    )
    west, east = ring(own, "lon", 1), ring(own, "lon", -1)
    forcing = ((levels, columns), bf16)
    depth = max(-(-3 * levels // 16) * 16, 2 * B)
    f1, f2, f_edge, f_inner, cost, par = call(
        forward,
        [forcing] * 2
        + [((levels + 16, (HALO + 1) * B), bf16), ((levels, (HALO + 1) * B), bf16)]
        + [((8, B), f32), ((levels, 2 * B), f32)],
        [((depth, (count - 1) * B), bf16), ((levels, (count - 1) * B), f32), ((levels, (count - 1) * B), f32)],
        name="forward",
    )(counts, win_i, win_u, win_v, west, own, east, own_par, other_par, observed, live, weights)
    f_edge, f_inner = across(f_edge, pairs), swap(f_inner)
    win_1, win_2, f_own, total = call(
        forcing_windows, [win] * 2 + [packed, ((8, B), f32)], name="forcing"
    )(counts, f1, f2, f_edge, f_inner, cost)
    f_west, f_east = ring(f_own, "lon", 1), ring(f_own, "lon", -1)
    if along == 4:
        total = total + ring(total, "lon", 2) + f_west[:8] + f_east[:8]
    else:
        total = total + f_west[:8]
        shift = 2
        while shift < along:
            total = total + ring(total, "lon", shift)
            shift *= 2
    shift = 2
    while shift < tiles:
        total = total + ring(total, "lat", shift)
        shift *= 2
    total = total + swap(total)
    kept, sent = call(
        backward,
        [((part * half, B), f32)] * 2,
        [((depth, (count + 1) * B), bf16), ((levels, (count + 1) * B), f32), ((B, B), f32)],
        name="backward",
    )(counts, win_1, win_2, f_west, f_own, f_east, win_i, win_u, win_v, west, own, east, par)
    got = swap(sent)
    kept, got = kept.reshape(part, half, B), got.reshape(part, half, B)
    gradient = jnp.where(
        lax.axis_index("lev") == 0,
        jnp.concatenate([kept, got], axis=1),
        jnp.concatenate([got, kept], axis=1),
    )
    cells = increment.size * tiles * along * lax.axis_size("lev")
    return gradient, total[0, B - 1] / cells


def solution(mesh):
    for axis in ("lat", "lon"):
        assert mesh.shape[axis] & (mesh.shape[axis] - 1) == 0 and mesh.shape[axis] > 1
    in_specs = (
        P("lev", "lat", "lon"),
        P("lev", "lat", "lon"),
        P("lev", "lat", "lon"),
        P("lev"),
        P("lev", None),
        P(None, "lev"),
        P(),
        P(None, "lat", "lon", None, None, None),
        P("lat", "lon"),
        P("lat", "lon", None),
    )
    out_specs = (P("lev", "lat", "lon"), P())
    return jax.shard_map(body, mesh=mesh, in_specs=in_specs, out_specs=out_specs, check_vma=False)
```

```python
import functools

import jax
import jax.numpy as jnp
from jax import lax
from jax.experimental import pallas as pl
from jax.experimental.pallas import tpu as pltpu
from jax.sharding import PartitionSpec as P


B = 128
HALO = 2
GROUP = 4


def roll(x, shift):
    shift %= B
    return x if shift == 0 else pltpu.roll(x, shift, 1)


def lanes_of(level_count):
    return lax.broadcasted_iota(jnp.int32, (level_count, B), 1)


def block(ref, p):
    return ref[:, p * B : (p + 1) * B]


def pack_edges(fields, rows):
    packed = None
    for f, field in enumerate(fields):
        for q in range(rows):
            rolled = roll(field(q + 1), (f * rows + q) * GROUP + 2)
            if packed is None:
                lane = lanes_of(rolled.shape[0])
                packed = jnp.zeros_like(rolled)
            packed = jnp.where(lane // GROUP == f * rows + q, rolled, packed)
    return packed


def by_side(one, two):
    even = lax.axis_index("lon") % 2 == 0
    one, two = one[...].astype(jnp.float32), two[...].astype(jnp.float32)
    return jnp.where(even, one, two), jnp.where(even, two, one)


def side_block(one, own, two, f, rows):
    west, east = by_side(one, two)
    own = own[...].astype(jnp.float32)
    return side_block_of(west, own, east, f, rows)


def side_block_of(west, own, east, f, rows):
    lane = lanes_of(own.shape[0])
    first = lane % GROUP < 2
    low, high = -f * rows * GROUP, B // 2 - f * rows * GROUP
    western = jnp.where(first, roll(west, low), roll(own, low))
    eastern = jnp.where(first, roll(own, high), roll(east, high))
    return jnp.where(lane < B // 2, western, eastern)


def from_east(x, side, q):
    lane = lanes_of(x.shape[0])
    return jnp.where(lane == B - 1, roll(side, B - 1 - (B // 2 + q * GROUP + 2)), roll(x, -1))


def from_west(x, side, q):
    lane = lanes_of(x.shape[0])
    return jnp.where(lane == 0, roll(side, -(q * GROUP + 1)), roll(x, 1))


def put_split(stack, p, x):
    levels = x.shape[0]
    head = x.astype(jnp.bfloat16)
    stack[0:levels, p * B : (p + 1) * B] = head
    stack[levels : 2 * levels, p * B : (p + 1) * B] = head
    stack[2 * levels : 3 * levels, p * B : (p + 1) * B] = (x - head.astype(jnp.float32)).astype(jnp.bfloat16)


def clear_rest(stack, levels):
    if stack.shape[0] > 3 * levels:
        stack[3 * levels :, :] = jnp.zeros((stack.shape[0] - 3 * levels, stack.shape[1]), stack.dtype)


def split_matrix(matrix, levels):
    lane = lanes_of(levels)
    matrix = jnp.where(lane < levels, matrix, 0.0)
    head = matrix.astype(jnp.bfloat16).astype(jnp.float32)
    rest = matrix - head
    over = B - levels
    low = jnp.where(lane < levels, head, roll(rest, levels))
    high = jnp.where(lane < levels - over, roll(rest, -over), roll(head, levels - over))
    high = jnp.where(lane < 2 * levels - over, high, 0.0)
    return jnp.concatenate([low, high], axis=1).astype(jnp.bfloat16)


def as_column(row):
    shape = (row.shape[1], row.shape[1])
    square = lax.broadcasted_iota(jnp.int32, shape, 0) == lax.broadcasted_iota(jnp.int32, shape, 1)
    return jnp.sum(jnp.where(square, row, 0.0), axis=1, keepdims=True)


def pieces_of(x):
    head = x.astype(jnp.bfloat16).astype(jnp.float32)
    rest = (x - head).astype(jnp.bfloat16).astype(jnp.float32)
    return head, rest, x - head - rest


def carried_in(block, first):
    lane = lanes_of(block.shape[0])
    return jnp.sum(jnp.where((lane >= first) & (lane < first + 3), block, 0.0), axis=1, keepdims=True)


def spread_rows(rows, core, sources, level, mains, inner, edge):
    levels = sources[0].shape[0] // rows
    half = rows // 2
    at = pl.ds(level, levels)
    k = 0
    for src, main, width in zip(sources, mains, (HALO, 1, HALO)):
        for j in range(half):
            main[at, j * B : (j + 1) * B] = src[pl.ds(core * half + j, levels, stride=rows), :]
        for j in range(width):
            near = jnp.where(core == 0, half + j, half - width + j)
            far = jnp.where(core == 0, j, rows - width + j)
            lanes = slice(k * B, (k + 1) * B)
            inner[at, lanes] = src[pl.ds(near, levels, stride=rows), :]
            edge[at, lanes] = src[pl.ds(far, levels, stride=rows), :].astype(edge.dtype)
            k += 1


def arrange_own(
    rows, counts, lookup, weight, mixing, diffusion, radiance, inc, u, v,
    main_i, main_u, main_v, inner, edge, par, places, weights,
    count_at, lookup_at, weight_at, mixing_at, diffusion_at, radiance_at, inc_at, u_at, v_at, arrived,
):
    core = lax.axis_index("lev")
    here = (count_at, lookup_at, weight_at, mixing_at, diffusion_at, radiance_at, inc_at, u_at, v_at)
    copies = [
        pltpu.make_async_copy(src, dst, arrived.at[i])
        for i, (src, dst) in enumerate(
            zip((counts, lookup, weight, mixing, diffusion, radiance, inc, u, v), here)
        )
    ]
    for copy in copies:
        copy.start()
    for copy in copies[:6]:
        copy.wait()
    slots, width = lookup.shape
    columns = main_i.shape[1]
    slot = lax.broadcasted_iota(jnp.int32, (slots, width), 0)
    places[...] = jnp.where(slot < count_at[0, 0], lookup_at[...] - core * columns, -1)
    part, levels = mixing.shape
    weights[...] = jnp.broadcast_to(as_column(weight_at[...]), weights.shape)
    par[:, :B] = jnp.broadcast_to(as_column(diffusion_at[...]), (part, B))
    par[:, :levels] = mixing_at[...]
    par[:, B:] = radiance_at[...].astype(jnp.float32)
    for copy in copies[6:]:
        copy.wait()
    level = pl.multiple_of(core * part, 8)
    spread_rows(rows, core, (inc_at, u_at, v_at), level, (main_i, main_u, main_v), inner, edge)


def arrange_other(
    rows, inc, u, v, main_i0, main_u0, main_v0, inner0, edge0, main_i, main_u, main_v, inner, edge
):
    core = lax.axis_index("lev")
    level = pl.multiple_of((1 - core) * (inc.shape[0] // rows), 8)
    spread_rows(rows, core, (inc, u, v), level, (main_i, main_u, main_v), inner, edge)


def one_hot(after, places, hot):
    columns = hot.shape[0]
    slots, width = places.shape
    index = lax.broadcasted_iota(jnp.int32, (columns, width), 0)
    for s in range(slots):
        hot[:, s * width : (s + 1) * width] = jnp.where(index == places[s : s + 1, :], 1.0, 0.0).astype(jnp.bfloat16)


def by_column(after, hot, observed, out, live, stacked):
    steps, slots, channels, width = observed.shape
    for s in range(slots):
        for t in range(steps):
            stacked[t * channels : (t + 1) * channels, s * width : (s + 1) * width] = observed[t, s]
    tail = stacked.shape[0] - steps * channels
    stacked[steps * channels :, :] = jnp.ones((tail, slots * width), jnp.bfloat16)
    moved = lax.dot_general(
        stacked[...], hot[...], (((1,), (1,)), ((), ())), preferred_element_type=jnp.float32
    )
    out[...] = moved[: steps * channels].astype(jnp.bfloat16)
    live[...] = moved[steps * channels : steps * channels + 8]


def flags():
    core, lat = lax.axis_index("lev"), lax.axis_index("lat")
    first = (core == 1) | (lat > 0)
    final = (core == 0) | (lat < lax.axis_size("lat") - 1)
    return core, first, final


def fill_halo(win, near, far, low, width):
    count = win.shape[1] // B
    win[:, (HALO - width) * B : HALO * B] = jnp.where(low, far, near)
    win[:, (count - HALO) * B : (count - HALO + width) * B] = jnp.where(low, near, far)


def windows(main_i, main_u, main_v, inner, edge, after, win_i, win_u, win_v, packed):
    low = lax.axis_index("lev") == 0
    count = win_i.shape[1] // B
    k = 0
    for main, win, width in ((main_i, win_i, HALO), (main_u, win_u, 1), (main_v, win_v, HALO)):
        win[:, HALO * B : (count - HALO) * B] = main[...]
        span = slice(k * B, (k + width) * B)
        fill_halo(win, inner[:, span], edge[:, span].astype(jnp.float32), low, width)
        k += width
    packed[...] = pack_edges(
        [functools.partial(block, win) for win in (win_i, win_u, win_v)], count - 2
    ).astype(packed.dtype)


def smooth(x, north, south, east, west, diff, u, v):
    return (
        x
        + diff * ((north + south) + (east + west) - 4.0 * x)
        - 0.5 * u * (east - west)
        - 0.5 * v * (north - south)
    )


def forward(
    win_i, win_u, win_v, west, own, east, own_par, other_par, observed, live, weights,
    f1, f2, edge, inner, cost, par, stack, plain, state,
):
    core, is_first, is_final = flags()
    part = own_par.shape[0]
    par[pl.ds(pl.multiple_of(core * part, 8), part), :] = own_par[...]
    par[pl.ds(pl.multiple_of((1 - core) * part, 8), part), :] = other_par[...]
    levels = par.shape[0]
    count = win_i.shape[1] // B
    rows = count - 2
    half = rows - 2
    diff = par[:, levels : levels + 1]
    coupling = split_matrix(par[:, :B], levels)
    radiance = par[:, B:].astype(jnp.bfloat16)
    channels = radiance.shape[1]
    scale = weights[:, :1]
    clear_rest(stack, levels)
    sides = [side_block(west, own, east, f, rows) for f in range(3)]
    for q in range(rows):
        p = q + 1
        x = block(win_i, p)
        s = smooth(
            x, block(win_i, p + 1), block(win_i, p - 1), from_east(x, sides[0], q), from_west(x, sides[0], q),
            diff, block(win_u, p), block(win_v, p),
        )
        plain[:, q * B : (q + 1) * B] = s
        put_split(stack, q, s)
    x = sides[0]
    s = smooth(x, roll(x, -GROUP), roll(x, GROUP), roll(x, -1), roll(x, 1), diff, sides[1], sides[2])
    plain[:, rows * B :] = s
    put_split(stack, rows, s)
    state[...] = plain[...] + jnp.dot(coupling, stack[...], preferred_element_type=jnp.float32)
    first, final = (rows - 1) * B, rows * B
    state[:, :B] = jnp.where(is_first, state[:, :B], 0.0)
    state[:, first:final] = jnp.where(is_final, state[:, first:final], 0.0)

    def observe(profile, t, out):
        evolved = lax.dot_general(
            radiance, profile, (((0,), (0,)), ((), ())), preferred_element_type=jnp.float32
        )
        departure = evolved - observed[t * channels : (t + 1) * channels, :].astype(jnp.float32)
        misfit = live[0:1, :] * departure
        scaled = scale * misfit
        back = jnp.dot(radiance, scaled.astype(jnp.bfloat16), preferred_element_type=jnp.float32)
        out[...] = back.astype(jnp.bfloat16)
        return jnp.sum(misfit * scaled, keepdims=True)

    total = observe(state[:, B : (half + 1) * B].astype(jnp.bfloat16), 0, f1)
    side = state[:, rows * B :]
    for q in range(1, rows - 1):
        x = block(state, q)
        s = smooth(
            x, block(state, q + 1), block(state, q - 1), from_east(x, side, q), from_west(x, side, q),
            diff, block(win_u, q + 1), block(win_v, q + 1),
        )
        plain[:, (q - 1) * B : q * B] = s
        put_split(stack, q - 1, s)
    end = plain[:, : half * B] + jnp.dot(coupling, stack[:, : half * B], preferred_element_type=jnp.float32)
    total = total + observe(end.astype(jnp.bfloat16), 1, f2)
    whole = win_i[:, HALO * B : (count - HALO) * B]
    total = 0.5 * (total + jnp.sum(whole * whole, keepdims=True))
    cost[...] = jnp.broadcast_to(total, cost.shape)
    low = core == 0
    k = 0
    for f, width in ((f2, HALO), (f1, 1)):
        head, tail = f[:, : width * B].astype(jnp.float32), f[:, (half - width) * B :].astype(jnp.float32)
        edge[:levels, k * B : (k + width) * B] = jnp.where(low, head, tail).astype(jnp.bfloat16)
        inner[:, k * B : (k + width) * B] = jnp.where(low, tail, head).astype(jnp.bfloat16)
        k += width
    tail = edge.shape[0] - levels
    lane = lanes_of(tail)
    carried = jnp.zeros((tail, B), jnp.float32)
    for i, piece in enumerate(pieces_of(total)):
        carried = jnp.where(lane == i, piece, carried)
    edge[levels:, :B] = carried.astype(jnp.bfloat16)
    edge[levels:, B:] = jnp.zeros((tail, edge.shape[1] - B), jnp.bfloat16)


def forcing_windows(f1, f2, edge, inner, cost, win_1, win_2, packed, total):
    core, is_first, is_final = flags()
    low = core == 0
    inside = is_first & is_final
    levels = f1.shape[0]
    count = win_1.shape[1] // B
    k = 0
    for f, win, width in ((f2, win_2, HALO), (f1, win_1, 1)):
        win[:, HALO * B : (count - HALO) * B] = f[...].astype(jnp.float32)
        span = slice(k * B, (k + width) * B)
        far = jnp.where(inside, edge[:levels, span].astype(jnp.float32), 0.0)
        fill_halo(win, inner[:, span].astype(jnp.float32), far, low, width)
        k += width
    both = pack_edges([functools.partial(block, win) for win in (win_2, win_1)], count - 2)
    here = cost[...] + carried_in(edge[levels:, :B].astype(jnp.float32), 0)[: cost.shape[0]]
    total[...] = here
    lane = lanes_of(both.shape[0])
    for i, piece in enumerate(pieces_of(here[0:1, :])):
        both = jnp.where(lane == B - 3 + i, piece, both)
    packed[...] = both.astype(packed.dtype)


def add_sides(two_sided, cost, cost_2, west, east, total):
    west, east = by_side(west, east)
    here = cost[...] + carried_in(west, B - 3)[: cost.shape[0]]
    if two_sided:
        here = here + cost_2[...] + carried_in(east, B - 3)[: cost.shape[0]]
    total[...] = here


def backward(
    win_1, win_2, fwest, fown, feast, win_i, win_u, win_v, west, own, east, par, after,
    kept, sent, stack, coupled, square,
):
    core, is_first, is_final = flags()
    levels = par.shape[0]
    count = win_i.shape[1] // B
    rows = count - 2
    half = rows - 2
    diff = par[:, levels : levels + 1]
    middle = 1.0 - 4.0 * diff
    square[...] = jnp.zeros(square.shape, jnp.float32)
    square[:levels, :] = jnp.where(lanes_of(levels) < levels, par[:, :B], 0.0)
    coupling = split_matrix(jnp.transpose(square[...])[:levels], levels)
    clear_rest(stack, levels)
    f_sides = [side_block(fwest, fown, feast, f, rows) for f in range(2)]
    sides = [side_block(west, own, east, f, rows) for f in range(3)]
    for p in range(count):
        x = block(win_2, p)
        coupled[:, p * B : (p + 1) * B] = x
        put_split(stack, p, x)
    coupled[:, count * B :] = f_sides[0]
    put_split(stack, count, f_sides[0])
    coupled[...] = coupled[...] + jnp.dot(coupling, stack[...], preferred_element_type=jnp.float32)

    def spread(p, q, side):
        x = block(coupled, p)
        north = (diff + 0.5 * block(win_v, q + 2)) * block(coupled, p + 1)
        south = (diff - 0.5 * block(win_v, q)) * block(coupled, p - 1)
        u = 0.5 * block(win_u, q + 1)
        side_east = (diff + 0.5 * sides[1]) * side
        side_west = (diff - 0.5 * sides[1]) * side
        return (
            middle * x + north + south + from_east((diff + u) * x, side_east, q)
            + from_west((diff - u) * x, side_west, q)
        )

    side = coupled[:, count * B :]
    after = []
    side_v, side_u = 0.5 * sides[2], 0.5 * sides[1]
    result = (
        middle * side
        + roll((diff + side_v) * side, -GROUP)
        + roll((diff - side_v) * side, GROUP)
        + roll((diff + side_u) * side, -1)
        + roll((diff - side_u) * side, 1)
        + f_sides[1]
    )
    for q in range(rows):
        after.append(spread(q + 1, q, side) + block(win_1, q + 1))
    after[0] = jnp.where(is_first, after[0], 0.0)
    after[-1] = jnp.where(is_final, after[-1], 0.0)
    for q in range(rows):
        coupled[:, (q + 1) * B : (q + 2) * B] = after[q]
        put_split(stack, q, after[q])
    coupled[:, count * B :] = result
    put_split(stack, rows, result)
    mixed = jnp.dot(coupling, stack[:, : (rows + 1) * B], preferred_element_type=jnp.float32)
    coupled[:, B : (rows + 1) * B] = coupled[:, B : (rows + 1) * B] + mixed[:, : rows * B]
    side = coupled[:, count * B :] + mixed[:, rows * B :]
    low = core == 0
    part = levels // 2
    for j in range(half):
        value = block(win_i, j + HALO) + spread(j + HALO, j + 1, side)
        kept[pl.ds(j, part, stride=half), :] = jnp.where(low, value[:part], value[part:])
        sent[pl.ds(j, part, stride=half), :] = jnp.where(low, value[part:], value[:part])


def finish(cells, kept, got, cost, cost_2, gradient, value, done):
    core = lax.axis_index("lev")
    half = kept.shape[1]
    copies = [
        pltpu.make_async_copy(src, gradient.at[:, pl.ds(pl.multiple_of(at * half, 8), half), :], done.at[i])
        for i, (src, at) in enumerate(((kept, core), (got, 1 - core)))
    ]
    for copy in copies:
        copy.start()
    value[0, 0] = jnp.max(cost[0:1, :] + cost_2[0:1, :]) / cells
    for copy in copies:
        copy.wait()


def call(kernel, outs, scratch=(), aliases=None, from_hbm=False, to_hbm=False, flops=10**9):
    vmem = pl.BlockSpec(memory_space=pltpu.VMEM)
    hbm = pl.BlockSpec(memory_space=pltpu.HBM)

    def run(*operands):
        if from_hbm:
            operands = [x if x.size == 1 else pltpu.with_memory_space_constraint(x, pltpu.HBM) for x in operands]
        return pl.pallas_call(
            kernel,
            out_shape=[jax.ShapeDtypeStruct(shape, dtype) for shape, dtype in outs],
            in_specs=[hbm if from_hbm else vmem] * len(operands),
            out_specs=[pl.BlockSpec(memory_space=pl.ANY), pl.BlockSpec(memory_space=pltpu.SMEM)]
            if to_hbm
            else [vmem] * len(outs),
            scratch_shapes=[
                shape if dtype is None else pltpu.VMEM(shape, dtype) for shape, dtype in scratch
            ],
            input_output_aliases=aliases or {},
            cost_estimate=pl.CostEstimate(flops=flops, bytes_accessed=0, transcendentals=0),
            compiler_params=pltpu.CompilerParams(vmem_limit_bytes=24 * 2**20),
        )(*operands)

    return run


def beside(x):
    count = lax.axis_size("lon")
    got = []
    for first in (1, 0):
        pairs = [((2 * i + first) % count, (2 * i + first + 1) % count) for i in range(count // 2)]
        got.append(lax.ppermute(x, "lon", pairs + [(b, a) for a, b in pairs] if count > 2 else [(0, 1), (1, 0)]))
    return got


def ring(x, axis, shift):
    count = lax.axis_size(axis)
    return lax.ppermute(x, axis, [(i, (i + shift) % count) for i in range(count)])


def body(
    increment, wind_u, wind_v, diffusion, mixing, jacobian, obs_weight, innovation, counts, column_lookup
):
    part, rows, width = increment.shape
    levels = mixing.shape[1]
    steps, channels = innovation.shape[0], innovation.shape[-2]
    slots = innovation.shape[3]
    assert width == B and steps == HALO and levels == 2 * part
    half = rows // 2
    count = half + 2 * HALO
    columns = half * B
    f32, bf16 = jnp.float32, jnp.bfloat16
    tiles, along = lax.axis_size("lat"), lax.axis_size("lon")
    pairs = [(2 * i + 1, (2 * i + 2) % (2 * tiles)) for i in range(tiles)]
    pairs = pairs + [(b, a) for a, b in pairs]
    inside = [(a, b) for a, b in pairs if abs(a - b) == 1]

    def swap(x):
        return lax.ppermute(x, "lev", [(0, 1), (1, 0)])

    def across(x, which):
        return lax.ppermute(x, ("lat", "lev"), which)

    fields = [x.reshape(part * rows, B) for x in (increment, wind_u, wind_v)]
    others = [swap(x) for x in fields]
    halo = 2 * HALO + 1
    main = ((levels, columns), f32)
    groups = [main] * 3 + [((levels, halo * B), f32), ((levels, halo * B), bf16)]
    win = ((levels, count * B), f32)
    packed = ((levels, B), bf16)
    field = ((part * rows, B), f32)
    scalar = ((8, B), f32)
    waits = pltpu.SemaphoreType.DMA
    *sorted_rows, own_par, places, weights = call(
        functools.partial(arrange_own, rows),
        groups + [((part, 2 * B), f32), ((slots, B), jnp.int32), ((channels, B), f32)],
        [(pltpu.SMEM((1, 1), jnp.int32), None), ((slots, B), jnp.int32), ((1, channels), f32)]
        + [((part, levels), f32), ((1, part), f32), ((part, channels), bf16)]
        + [field] * 3
        + [(waits((9,)), None)],
        from_hbm=True,
    )(
        counts, column_lookup.reshape(slots, B), obs_weight.reshape(1, -1), mixing, diffusion.reshape(1, -1),
        jacobian.T, *fields,
    )
    *mains, inner, edge = call(
        functools.partial(arrange_other, rows), groups,
        aliases={3 + i: i for i in range(5)},
    )(*others, *sorted_rows)
    edge = across(edge, inside)
    other_par = swap(own_par)
    (hot,) = call(one_hot, [((columns, slots * B), bf16)])(inner, places)
    win_i, win_u, win_v, own = call(windows, [win] * 3 + [packed])(*mains, inner, edge, hot)
    observed, live = call(
        by_column,
        [((steps * channels, columns), bf16), ((8, columns), f32)],
        [((steps * channels + 16, slots * B), bf16)],
    )(own, hot, innovation.reshape(steps, slots, channels, B))
    west, east = beside(own)
    forcing = ((levels, columns), bf16)
    depth = max(-(-3 * levels // 16) * 16, 2 * B)
    f1, f2, f_edge, f_inner, cost, par = call(
        forward,
        [forcing] * 2
        + [((levels + 16, (HALO + 1) * B), bf16), ((levels, (HALO + 1) * B), bf16)]
        + [scalar, ((levels, 2 * B), f32)],
        [((depth, (count - 1) * B), bf16), ((levels, (count - 1) * B), f32), ((levels, (count - 1) * B), f32)],
    )(win_i, win_u, win_v, west, own, east, own_par, other_par, observed, live, weights)
    f_edge, f_inner = across(f_edge, pairs), swap(f_inner)
    win_1, win_2, f_own, total = call(forcing_windows, [win] * 2 + [packed, scalar])(f1, f2, f_edge, f_inner, cost)
    f_west, f_east = beside(f_own)
    few_points = along == 4
    total_2 = ring(total, "lon", 2) if few_points else total
    (total,) = call(functools.partial(add_sides, few_points), [scalar], flops=10**7)(total, total_2, f_west, f_east)
    more = ring(total, "lat", 2) if tiles > 2 else None
    kept, sent = call(
        backward,
        [((part * half, B), f32)] * 2,
        [((depth, (count + 1) * B), bf16), ((levels, (count + 1) * B), f32), ((B, B), f32)],
    )(win_1, win_2, f_west, f_own, f_east, win_i, win_u, win_v, west, own, east, par, total)
    if more is not None:
        total = total + more
    for axis, size, few in (("lat", tiles, False), ("lon", along, few_points)):
        shift = 4 if axis == "lat" else 2
        while shift < size and not few:
            total = total + ring(total, axis, shift)
            shift *= 2
    cells = increment.size * tiles * along * lax.axis_size("lev")
    gradient, value = call(
        functools.partial(finish, float(cells)),
        [(increment.shape, f32), ((1, 1), f32)],
        [(waits((2,)), None)],
        to_hbm=True,
    )(kept.reshape(part, half, B), swap(sent).reshape(part, half, B), total, swap(total))
    return gradient, value.reshape(())


def solution(mesh):
    for axis in ("lat", "lon"):
        assert mesh.shape[axis] & (mesh.shape[axis] - 1) == 0 and mesh.shape[axis] > 1
    in_specs = (
        P("lev", "lat", "lon"),
        P("lev", "lat", "lon"),
        P("lev", "lat", "lon"),
        P("lev"),
        P("lev", None),
        P(None, "lev"),
        P(),
        P(None, "lat", "lon", None, None, None),
        P("lat", "lon"),
        P("lat", "lon", None),
    )
    out_specs = (P("lev", "lat", "lon"), P())

    return jax.shard_map(body, mesh=mesh, in_specs=in_specs, out_specs=out_specs, check_vma=False)
```

```python
import functools

import jax
import jax.numpy as jnp
from jax import lax
from jax.experimental import pallas as pl
from jax.experimental.pallas import tpu as pltpu
from jax.sharding import PartitionSpec as P


B = 128
HALO = 2
GROUP = 4


def roll(x, shift):
    shift %= B
    return x if shift == 0 else pltpu.roll(x, shift, 1)


def lanes_of(level_count):
    return lax.broadcasted_iota(jnp.int32, (level_count, B), 1)


def block(ref, p):
    return ref[:, p * B : (p + 1) * B]


def pack_edges(fields, rows):
    packed = None
    for f, field in enumerate(fields):
        for q in range(rows):
            rolled = roll(field(q + 1), (f * rows + q) * GROUP + 2)
            if packed is None:
                lane = lanes_of(rolled.shape[0])
                packed = jnp.zeros_like(rolled)
            packed = jnp.where(lane // GROUP == f * rows + q, rolled, packed)
    return packed


def by_side(one, two):
    even = lax.axis_index("lon") % 2 == 0
    one, two = one[...].astype(jnp.float32), two[...].astype(jnp.float32)
    return jnp.where(even, one, two), jnp.where(even, two, one)


def side_block(one, own, two, f, rows):
    west, east = by_side(one, two)
    own = own[...].astype(jnp.float32)
    return side_block_of(west, own, east, f, rows)


def side_block_of(west, own, east, f, rows):
    lane = lanes_of(own.shape[0])
    first = lane % GROUP < 2
    low, high = -f * rows * GROUP, B // 2 - f * rows * GROUP
    western = jnp.where(first, roll(west, low), roll(own, low))
    eastern = jnp.where(first, roll(own, high), roll(east, high))
    return jnp.where(lane < B // 2, western, eastern)


def from_east(x, side, q):
    lane = lanes_of(x.shape[0])
    return jnp.where(lane == B - 1, roll(side, B - 1 - (B // 2 + q * GROUP + 2)), roll(x, -1))


def from_west(x, side, q):
    lane = lanes_of(x.shape[0])
    return jnp.where(lane == 0, roll(side, -(q * GROUP + 1)), roll(x, 1))


def put_split(stack, p, x):
    levels = x.shape[0]
    head = x.astype(jnp.bfloat16)
    stack[0:levels, p * B : (p + 1) * B] = head
    stack[levels : 2 * levels, p * B : (p + 1) * B] = head
    stack[2 * levels : 3 * levels, p * B : (p + 1) * B] = (x - head.astype(jnp.float32)).astype(jnp.bfloat16)


def clear_rest(stack, levels):
    if stack.shape[0] > 3 * levels:
        stack[3 * levels :, :] = jnp.zeros((stack.shape[0] - 3 * levels, stack.shape[1]), stack.dtype)


def split_matrix(matrix, levels):
    lane = lanes_of(levels)
    matrix = jnp.where(lane < levels, matrix, 0.0)
    head = matrix.astype(jnp.bfloat16).astype(jnp.float32)
    rest = matrix - head
    over = B - levels
    low = jnp.where(lane < levels, head, roll(rest, levels))
    high = jnp.where(lane < levels - over, roll(rest, -over), roll(head, levels - over))
    high = jnp.where(lane < 2 * levels - over, high, 0.0)
    return jnp.concatenate([low, high], axis=1).astype(jnp.bfloat16)


def as_column(row):
    shape = (row.shape[1], row.shape[1])
    square = lax.broadcasted_iota(jnp.int32, shape, 0) == lax.broadcasted_iota(jnp.int32, shape, 1)
    return jnp.sum(jnp.where(square, row, 0.0), axis=1, keepdims=True)


def pieces_of(x):
    head = x.astype(jnp.bfloat16).astype(jnp.float32)
    rest = (x - head).astype(jnp.bfloat16).astype(jnp.float32)
    return head, rest, x - head - rest


def carried_in(block, first):
    lane = lanes_of(block.shape[0])
    return jnp.sum(jnp.where((lane >= first) & (lane < first + 3), block, 0.0), axis=1, keepdims=True)


def spread_rows(rows, core, sources, level, mains, inner, edge):
    levels = sources[0].shape[0] // rows
    half = rows // 2
    at = pl.ds(level, levels)
    k = 0
    for src, main, width in zip(sources, mains, (HALO, 1, HALO)):
        for j in range(half):
            main[at, j * B : (j + 1) * B] = src[pl.ds(core * half + j, levels, stride=rows), :]
        for j in range(width):
            near = jnp.where(core == 0, half + j, half - width + j)
            far = jnp.where(core == 0, j, rows - width + j)
            lanes = slice(k * B, (k + 1) * B)
            inner[at, lanes] = src[pl.ds(near, levels, stride=rows), :]
            edge[at, lanes] = src[pl.ds(far, levels, stride=rows), :].astype(edge.dtype)
            k += 1


def arrange_own(
    rows, lookup, weight, mixing, diffusion, radiance, inc, u, v,
    main_i, main_u, main_v, inner, edge, par, places, weights,
    lookup_at, weight_at, mixing_at, diffusion_at, radiance_at, inc_at, u_at, v_at, arrived,
):
    core = lax.axis_index("lev")
    here = (lookup_at, weight_at, mixing_at, diffusion_at, radiance_at, inc_at, u_at, v_at)
    copies = [
        pltpu.make_async_copy(src, dst, arrived.at[i])
        for i, (src, dst) in enumerate(
            zip((lookup, weight, mixing, diffusion, radiance, inc, u, v), here)
        )
    ]
    for copy in copies:
        copy.start()
    for copy in copies[:5]:
        copy.wait()
    places[...] = lookup_at[...] - core * main_i.shape[1]
    part, levels = mixing.shape
    weights[...] = jnp.broadcast_to(as_column(weight_at[...]), weights.shape)
    par[:, :B] = jnp.broadcast_to(as_column(diffusion_at[...]), (part, B))
    par[:, :levels] = mixing_at[...]
    par[:, B:] = radiance_at[...].astype(jnp.float32)
    for copy in copies[5:]:
        copy.wait()
    level = pl.multiple_of(core * part, 8)
    spread_rows(rows, core, (inc_at, u_at, v_at), level, (main_i, main_u, main_v), inner, edge)


def arrange_other(
    rows, inc, u, v, main_i0, main_u0, main_v0, inner0, edge0, main_i, main_u, main_v, inner, edge
):
    core = lax.axis_index("lev")
    level = pl.multiple_of((1 - core) * (inc.shape[0] // rows), 8)
    spread_rows(rows, core, (inc, u, v), level, (main_i, main_u, main_v), inner, edge)


def one_hot(counts, after, places, hot):
    columns = hot.shape[0]
    slots, width = places.shape
    index = lax.broadcasted_iota(jnp.int32, (columns, width), 0)
    for s in range(slots):
        place = jnp.where(s < counts[0, 0], places[s : s + 1, :], -1)
        hot[:, s * width : (s + 1) * width] = jnp.where(index == place, 1.0, 0.0).astype(jnp.bfloat16)


def by_column(after, hot, observed, out, live, stacked):
    steps, slots, channels, width = observed.shape
    for s in range(slots):
        for t in range(steps):
            stacked[t * channels : (t + 1) * channels, s * width : (s + 1) * width] = observed[t, s]
    tail = stacked.shape[0] - steps * channels
    stacked[steps * channels :, :] = jnp.ones((tail, slots * width), jnp.bfloat16)
    moved = lax.dot_general(
        stacked[...], hot[...], (((1,), (1,)), ((), ())), preferred_element_type=jnp.float32
    )
    out[...] = moved[: steps * channels].astype(jnp.bfloat16)
    live[...] = moved[steps * channels : steps * channels + 8]


def flags():
    core, lat = lax.axis_index("lev"), lax.axis_index("lat")
    first = (core == 1) | (lat > 0)
    final = (core == 0) | (lat < lax.axis_size("lat") - 1)
    return core, first, final


def fill_halo(win, near, far, low, width):
    count = win.shape[1] // B
    win[:, (HALO - width) * B : HALO * B] = jnp.where(low, far, near)
    win[:, (count - HALO) * B : (count - HALO + width) * B] = jnp.where(low, near, far)


def windows(main_i, main_u, main_v, inner, edge, after, win_i, win_u, win_v, packed):
    low = lax.axis_index("lev") == 0
    count = win_i.shape[1] // B
    k = 0
    for main, win, width in ((main_i, win_i, HALO), (main_u, win_u, 1), (main_v, win_v, HALO)):
        win[:, HALO * B : (count - HALO) * B] = main[...]
        span = slice(k * B, (k + width) * B)
        fill_halo(win, inner[:, span], edge[:, span].astype(jnp.float32), low, width)
        k += width
    packed[...] = pack_edges(
        [functools.partial(block, win) for win in (win_i, win_u, win_v)], count - 2
    ).astype(packed.dtype)


def smooth(x, north, south, east, west, diff, u, v):
    return (
        x
        + diff * ((north + south) + (east + west) - 4.0 * x)
        - 0.5 * u * (east - west)
        - 0.5 * v * (north - south)
    )


def forward(
    win_i, win_u, win_v, west, own, east, own_par, other_par, observed, live, weights,
    f1, f2, edge, inner, cost, par, stack, plain, state,
):
    core, is_first, is_final = flags()
    part = own_par.shape[0]
    par[pl.ds(pl.multiple_of(core * part, 8), part), :] = own_par[...]
    par[pl.ds(pl.multiple_of((1 - core) * part, 8), part), :] = other_par[...]
    levels = par.shape[0]
    count = win_i.shape[1] // B
    rows = count - 2
    half = rows - 2
    diff = par[:, levels : levels + 1]
    coupling = split_matrix(par[:, :B], levels)
    radiance = par[:, B:].astype(jnp.bfloat16)
    channels = radiance.shape[1]
    scale = weights[:, :1]
    clear_rest(stack, levels)
    sides = [side_block(west, own, east, f, rows) for f in range(3)]
    for q in range(rows):
        p = q + 1
        x = block(win_i, p)
        s = smooth(
            x, block(win_i, p + 1), block(win_i, p - 1), from_east(x, sides[0], q), from_west(x, sides[0], q),
            diff, block(win_u, p), block(win_v, p),
        )
        plain[:, q * B : (q + 1) * B] = s
        put_split(stack, q, s)
    x = sides[0]
    s = smooth(x, roll(x, -GROUP), roll(x, GROUP), roll(x, -1), roll(x, 1), diff, sides[1], sides[2])
    plain[:, rows * B :] = s
    put_split(stack, rows, s)
    state[...] = plain[...] + jnp.dot(coupling, stack[...], preferred_element_type=jnp.float32)
    first, final = (rows - 1) * B, rows * B
    state[:, :B] = jnp.where(is_first, state[:, :B], 0.0)
    state[:, first:final] = jnp.where(is_final, state[:, first:final], 0.0)

    def observe(profile, t, out):
        evolved = lax.dot_general(
            radiance, profile, (((0,), (0,)), ((), ())), preferred_element_type=jnp.float32
        )
        departure = evolved - observed[t * channels : (t + 1) * channels, :].astype(jnp.float32)
        misfit = live[0:1, :] * departure
        scaled = scale * misfit
        back = jnp.dot(radiance, scaled.astype(jnp.bfloat16), preferred_element_type=jnp.float32)
        out[...] = back.astype(jnp.bfloat16)
        return jnp.sum(misfit * scaled, keepdims=True)

    total = observe(state[:, B : (half + 1) * B].astype(jnp.bfloat16), 0, f1)
    side = state[:, rows * B :]
    for q in range(1, rows - 1):
        x = block(state, q)
        s = smooth(
            x, block(state, q + 1), block(state, q - 1), from_east(x, side, q), from_west(x, side, q),
            diff, block(win_u, q + 1), block(win_v, q + 1),
        )
        plain[:, (q - 1) * B : q * B] = s
        put_split(stack, q - 1, s)
    end = plain[:, : half * B] + jnp.dot(coupling, stack[:, : half * B], preferred_element_type=jnp.float32)
    total = total + observe(end.astype(jnp.bfloat16), 1, f2)
    whole = win_i[:, HALO * B : (count - HALO) * B]
    total = 0.5 * (total + jnp.sum(whole * whole, keepdims=True))
    cost[...] = jnp.broadcast_to(total, cost.shape)
    low = core == 0
    k = 0
    for f, width in ((f2, HALO), (f1, 1)):
        head, tail = f[:, : width * B].astype(jnp.float32), f[:, (half - width) * B :].astype(jnp.float32)
        edge[:levels, k * B : (k + width) * B] = jnp.where(low, head, tail).astype(jnp.bfloat16)
        inner[:, k * B : (k + width) * B] = jnp.where(low, tail, head).astype(jnp.bfloat16)
        k += width
    tail = edge.shape[0] - levels
    lane = lanes_of(tail)
    carried = jnp.zeros((tail, B), jnp.float32)
    for i, piece in enumerate(pieces_of(total)):
        carried = jnp.where(lane == i, piece, carried)
    edge[levels:, :B] = carried.astype(jnp.bfloat16)
    edge[levels:, B:] = jnp.zeros((tail, edge.shape[1] - B), jnp.bfloat16)


def forcing_windows(f1, f2, edge, inner, cost, win_1, win_2, packed, total):
    core, is_first, is_final = flags()
    low = core == 0
    inside = is_first & is_final
    levels = f1.shape[0]
    count = win_1.shape[1] // B
    k = 0
    for f, win, width in ((f2, win_2, HALO), (f1, win_1, 1)):
        win[:, HALO * B : (count - HALO) * B] = f[...].astype(jnp.float32)
        span = slice(k * B, (k + width) * B)
        far = jnp.where(inside, edge[:levels, span].astype(jnp.float32), 0.0)
        fill_halo(win, inner[:, span].astype(jnp.float32), far, low, width)
        k += width
    both = pack_edges([functools.partial(block, win) for win in (win_2, win_1)], count - 2)
    here = cost[...] + carried_in(edge[levels:, :B].astype(jnp.float32), 0)[: cost.shape[0]]
    total[...] = here
    lane = lanes_of(both.shape[0])
    for i, piece in enumerate(pieces_of(here[0:1, :])):
        both = jnp.where(lane == B - 3 + i, piece, both)
    packed[...] = both.astype(packed.dtype)


def add_sides(cost, one, two, *refs):
    *more, total = refs
    west, east = by_side(one, two)
    here = cost[...] + carried_in(west, B - 3)[: cost.shape[0]]
    if more:
        here = here + carried_in(east, B - 3)[: cost.shape[0]]
    for other in more:
        here = here + other[...]
    total[...] = here


def backward(
    win_1, win_2, fwest, fown, feast, win_i, win_u, win_v, west, own, east, par, after,
    kept, sent, stack, coupled, square,
):
    core, is_first, is_final = flags()
    levels = par.shape[0]
    count = win_i.shape[1] // B
    rows = count - 2
    half = rows - 2
    diff = par[:, levels : levels + 1]
    middle = 1.0 - 4.0 * diff
    square[...] = jnp.zeros(square.shape, jnp.float32)
    square[:levels, :] = jnp.where(lanes_of(levels) < levels, par[:, :B], 0.0)
    coupling = split_matrix(jnp.transpose(square[...])[:levels], levels)
    clear_rest(stack, levels)
    f_sides = [side_block(fwest, fown, feast, f, rows) for f in range(2)]
    sides = [side_block(west, own, east, f, rows) for f in range(3)]
    for p in range(count):
        x = block(win_2, p)
        coupled[:, p * B : (p + 1) * B] = x
        put_split(stack, p, x)
    coupled[:, count * B :] = f_sides[0]
    put_split(stack, count, f_sides[0])
    coupled[...] = coupled[...] + jnp.dot(coupling, stack[...], preferred_element_type=jnp.float32)

    def spread(p, q, side):
        x = block(coupled, p)
        north = (diff + 0.5 * block(win_v, q + 2)) * block(coupled, p + 1)
        south = (diff - 0.5 * block(win_v, q)) * block(coupled, p - 1)
        u = 0.5 * block(win_u, q + 1)
        side_east = (diff + 0.5 * sides[1]) * side
        side_west = (diff - 0.5 * sides[1]) * side
        return (
            middle * x + north + south + from_east((diff + u) * x, side_east, q)
            + from_west((diff - u) * x, side_west, q)
        )

    side = coupled[:, count * B :]
    after = []
    side_v, side_u = 0.5 * sides[2], 0.5 * sides[1]
    result = (
        middle * side
        + roll((diff + side_v) * side, -GROUP)
        + roll((diff - side_v) * side, GROUP)
        + roll((diff + side_u) * side, -1)
        + roll((diff - side_u) * side, 1)
        + f_sides[1]
    )
    for q in range(rows):
        after.append(spread(q + 1, q, side) + block(win_1, q + 1))
    after[0] = jnp.where(is_first, after[0], 0.0)
    after[-1] = jnp.where(is_final, after[-1], 0.0)
    for q in range(rows):
        coupled[:, (q + 1) * B : (q + 2) * B] = after[q]
        put_split(stack, q, after[q])
    coupled[:, count * B :] = result
    put_split(stack, rows, result)
    mixed = jnp.dot(coupling, stack[:, : (rows + 1) * B], preferred_element_type=jnp.float32)
    coupled[:, B : (rows + 1) * B] = coupled[:, B : (rows + 1) * B] + mixed[:, : rows * B]
    side = coupled[:, count * B :] + mixed[:, rows * B :]
    low = core == 0
    part = levels // 2
    for j in range(half):
        value = block(win_i, j + HALO) + spread(j + HALO, j + 1, side)
        kept[pl.ds(j, part, stride=half), :] = jnp.where(low, value[:part], value[part:])
        sent[pl.ds(j, part, stride=half), :] = jnp.where(low, value[part:], value[:part])


def write_half(kept, gradient, done):
    half = kept.shape[1]
    at = pl.multiple_of(lax.axis_index("lev") * half, 8)
    copy = pltpu.make_async_copy(kept, gradient.at[:, pl.ds(at, half), :], done)
    copy.start()
    copy.wait()


def finish(cells, got, cost, cost_2, begun, gradient, value, value_at, done):
    half = got.shape[1]
    at = pl.multiple_of((1 - lax.axis_index("lev")) * half, 8)
    copy = pltpu.make_async_copy(got, gradient.at[:, pl.ds(at, half), :], done.at[0])
    copy.start()
    value_at[0, 0] = jnp.max(cost[0:1, :] + cost_2[0:1, :]) / cells
    last = pltpu.make_async_copy(value_at, value, done.at[1])
    last.start()
    copy.wait()
    last.wait()


def call(kernel, outs, scratch=(), aliases=None, from_hbm=False, smem=0, spaces=None, results=None, flops=10**9):
    spaces, results = dict(spaces or {}), dict(results or {})
    spaces.update({i: pltpu.SMEM for i in range(smem)})

    def run(*operands):
        if from_hbm:
            operands = [pltpu.with_memory_space_constraint(x, pltpu.HBM) for x in operands]
        usual = pltpu.HBM if from_hbm else pltpu.VMEM
        return pl.pallas_call(
            kernel,
            out_shape=[jax.ShapeDtypeStruct(shape, dtype) for shape, dtype in outs],
            in_specs=[pl.BlockSpec(memory_space=spaces.get(i, usual)) for i in range(len(operands))],
            out_specs=[pl.BlockSpec(memory_space=results.get(i, pltpu.VMEM)) for i in range(len(outs))],
            scratch_shapes=[shape if dtype is None else pltpu.VMEM(shape, dtype) for shape, dtype in scratch],
            input_output_aliases=aliases or {},
            cost_estimate=pl.CostEstimate(flops=flops, bytes_accessed=0, transcendentals=0),
            compiler_params=pltpu.CompilerParams(vmem_limit_bytes=24 * 2**20),
        )(*operands)

    return run


def beside(x):
    count = lax.axis_size("lon")
    got = []
    for first in (1, 0):
        pairs = [((2 * i + first) % count, (2 * i + first + 1) % count) for i in range(count // 2)]
        got.append(lax.ppermute(x, "lon", pairs + [(b, a) for a, b in pairs] if count > 2 else [(0, 1), (1, 0)]))
    return got


def ring(x, axis, shift):
    count = lax.axis_size(axis)
    return lax.ppermute(x, axis, [(i, (i + shift) % count) for i in range(count)])


def body(
    increment, wind_u, wind_v, diffusion, mixing, jacobian, obs_weight, innovation, counts, column_lookup
):
    part, rows, width = increment.shape
    levels = mixing.shape[1]
    steps, channels = innovation.shape[0], innovation.shape[-2]
    slots = innovation.shape[3]
    assert width == B and steps == HALO and levels == 2 * part
    half = rows // 2
    count = half + 2 * HALO
    columns = half * B
    f32, bf16 = jnp.float32, jnp.bfloat16
    tiles, along = lax.axis_size("lat"), lax.axis_size("lon")
    pairs = [(2 * i + 1, (2 * i + 2) % (2 * tiles)) for i in range(tiles)]
    pairs = pairs + [(b, a) for a, b in pairs]
    inside = [(a, b) for a, b in pairs if abs(a - b) == 1]

    def swap(x):
        return lax.ppermute(x, "lev", [(0, 1), (1, 0)])

    def across(x, which):
        return lax.ppermute(x, ("lat", "lev"), which)

    fields = [x.reshape(part * rows, B) for x in (increment, wind_u, wind_v)]
    others = [swap(x) for x in fields]
    halo = 2 * HALO + 1
    main = ((levels, columns), f32)
    groups = [main] * 3 + [((levels, halo * B), f32), ((levels, halo * B), bf16)]
    win = ((levels, count * B), f32)
    packed = ((levels, B), bf16)
    field = ((part * rows, B), f32)
    scalar = ((8, B), f32)
    waits = pltpu.SemaphoreType.DMA
    *sorted_rows, own_par, places, weights = call(
        functools.partial(arrange_own, rows),
        groups + [((part, 2 * B), f32), ((slots, B), jnp.int32), ((channels, B), f32)],
        [((slots, B), jnp.int32), ((1, channels), f32)]
        + [((part, levels), f32), ((1, part), f32), ((part, channels), bf16)]
        + [field] * 3
        + [(waits((8,)), None)],
        from_hbm=True,
    )(
        column_lookup.reshape(slots, B), obs_weight.reshape(1, -1), mixing, diffusion.reshape(1, -1),
        jacobian.T, *fields,
    )
    *mains, inner, edge = call(
        functools.partial(arrange_other, rows), groups,
        aliases={3 + i: i for i in range(5)},
    )(*others, *sorted_rows)
    edge = across(edge, inside)
    other_par = swap(own_par)
    (hot,) = call(one_hot, [((columns, slots * B), bf16)], smem=1)(counts, inner, places)
    win_i, win_u, win_v, own = call(windows, [win] * 3 + [packed])(*mains, inner, edge, hot)
    observed, live = call(
        by_column,
        [((steps * channels, columns), bf16), ((8, columns), f32)],
        [((steps * channels + 16, slots * B), bf16)],
    )(own, hot, innovation.reshape(steps, slots, channels, B))
    west, east = beside(own)
    forcing = ((levels, columns), bf16)
    depth = max(-(-3 * levels // 16) * 16, 2 * B)
    f1, f2, f_edge, f_inner, cost, par = call(
        forward,
        [forcing] * 2
        + [((levels + 16, (HALO + 1) * B), bf16), ((levels, (HALO + 1) * B), bf16)]
        + [scalar, ((levels, 2 * B), f32)],
        [((depth, (count - 1) * B), bf16), ((levels, (count - 1) * B), f32), ((levels, (count - 1) * B), f32)],
    )(win_i, win_u, win_v, west, own, east, own_par, other_par, observed, live, weights)
    few_points = along == 4
    f_edge, f_inner = across(f_edge, pairs), swap(f_inner)
    far_cost = ring(cost, "lon", 2) if few_points else None
    win_1, win_2, f_own, total = call(forcing_windows, [win] * 2 + [packed, scalar])(f1, f2, f_edge, f_inner, cost)
    f_west, f_east = beside(f_own)
    more = []
    if few_points:
        more = [far_cost, across(far_cost, pairs)]
    (total,) = call(add_sides, [scalar], flops=10**7)(total, f_west, f_east, *more)
    more = ring(total, "lat", 2) if tiles > 2 else None
    kept, sent = call(
        backward,
        [((part * half, B), f32)] * 2,
        [((depth, (count + 1) * B), bf16), ((levels, (count + 1) * B), f32), ((B, B), f32)],
    )(win_1, win_2, f_west, f_own, f_east, win_i, win_u, win_v, west, own, east, par, total)
    if more is not None:
        total = total + more
    for axis, size, few in (("lat", tiles, False), ("lon", along, few_points)):
        shift = 4 if axis == "lat" else 2
        while shift < size and not few:
            total = total + ring(total, axis, shift)
            shift *= 2
    cells = increment.size * tiles * along * lax.axis_size("lev")
    got = swap(sent).reshape(part, half, B)
    total_2 = swap(total)
    (begun,) = call(
        write_half, [(increment.shape, f32)], [(waits(()), None)], results={0: pl.ANY}
    )(kept.reshape(part, half, B))
    gradient, value = call(
        functools.partial(finish, float(cells)),
        [(increment.shape, f32), ((1, 1), f32)],
        [(pltpu.SMEM((1, 1), f32), None), (waits((2,)), None)],
        spaces={3: pl.ANY},
        results={0: pl.ANY, 1: pl.ANY},
        aliases={3: 0},
    )(got, total, total_2, begun)
    return gradient, value.reshape(())


def solution(mesh):
    for axis in ("lat", "lon"):
        assert mesh.shape[axis] & (mesh.shape[axis] - 1) == 0 and mesh.shape[axis] > 1
    in_specs = (
        P("lev", "lat", "lon"),
        P("lev", "lat", "lon"),
        P("lev", "lat", "lon"),
        P("lev"),
        P("lev", None),
        P(None, "lev"),
        P(),
        P(None, "lat", "lon", None, None, None),
        P("lat", "lon"),
        P("lat", "lon", None),
    )
    out_specs = (P("lev", "lat", "lon"), P())

    return jax.shard_map(body, mesh=mesh, in_specs=in_specs, out_specs=out_specs, check_vma=False)
```

```python
import functools

import jax
import jax.numpy as jnp
from jax import lax
from jax.experimental import pallas as pl
from jax.experimental.pallas import tpu as pltpu
from jax.sharding import PartitionSpec as P


B = 128
HALO = 2
GROUP = 4


def roll(x, shift):
    shift %= B
    return x if shift == 0 else pltpu.roll(x, shift, 1)


def lanes_of(level_count):
    return lax.broadcasted_iota(jnp.int32, (level_count, B), 1)


def block(ref, p):
    return ref[:, p * B : (p + 1) * B]


def pack_edges(fields, rows):
    packed = None
    for f, field in enumerate(fields):
        for q in range(rows):
            rolled = roll(field(q + 1), (f * rows + q) * GROUP + 2)
            if packed is None:
                lane = lanes_of(rolled.shape[0])
                packed = jnp.zeros_like(rolled)
            packed = jnp.where(lane // GROUP == f * rows + q, rolled, packed)
    return packed


def by_side(one, two):
    even = lax.axis_index("lon") % 2 == 0
    one, two = one[...].astype(jnp.float32), two[...].astype(jnp.float32)
    return jnp.where(even, one, two), jnp.where(even, two, one)


def side_block(one, own, two, f, rows):
    west, east = by_side(one, two)
    own = own[...].astype(jnp.float32)
    return side_block_of(west, own, east, f, rows)


def side_block_of(west, own, east, f, rows):
    lane = lanes_of(own.shape[0])
    first = lane % GROUP < 2
    low, high = -f * rows * GROUP, B // 2 - f * rows * GROUP
    western = jnp.where(first, roll(west, low), roll(own, low))
    eastern = jnp.where(first, roll(own, high), roll(east, high))
    return jnp.where(lane < B // 2, western, eastern)


def both_ends(from_east, from_west):
    lane = lanes_of(from_east.shape[0])
    return jnp.where(lane % GROUP == 0, roll(from_east, -(B // 2 + 2)), from_west)


def beyond(ends, q):
    return roll(ends, B - 1 - q * GROUP)


def from_east(x, ends):
    return jnp.where(lanes_of(x.shape[0]) == B - 1, ends, roll(x, -1))


def from_west(x, ends):
    return jnp.where(lanes_of(x.shape[0]) == 0, ends, roll(x, 1))


def put(stack, p, x):
    levels = x.shape[0]
    head = x.astype(jnp.bfloat16)
    stack[0:levels, p * B : (p + 1) * B] = head
    stack[levels : 2 * levels, p * B : (p + 1) * B] = head
    stack[2 * levels : 3 * levels, p * B : (p + 1) * B] = (x - head.astype(jnp.float32)).astype(jnp.bfloat16)


def clear_rest(stack, levels):
    if stack.shape[0] > 3 * levels:
        stack[3 * levels :, :] = jnp.zeros((stack.shape[0] - 3 * levels, stack.shape[1]), stack.dtype)


def split_matrix(matrix, levels):
    lane = lanes_of(levels)
    matrix = jnp.where(lane < levels, matrix, 0.0)
    head = matrix.astype(jnp.bfloat16).astype(jnp.float32)
    rest = matrix - head
    over = B - levels
    low = jnp.where(lane < levels, head, roll(rest, levels))
    high = jnp.where(lane < levels - over, roll(rest, -over), roll(head, levels - over))
    high = jnp.where(lane < 2 * levels - over, high, 0.0)
    return jnp.concatenate([low, high], axis=1).astype(jnp.bfloat16)


def as_column(row):
    shape = (row.shape[1], row.shape[1])
    square = lax.broadcasted_iota(jnp.int32, shape, 0) == lax.broadcasted_iota(jnp.int32, shape, 1)
    return jnp.sum(jnp.where(square, row, 0.0), axis=1, keepdims=True)


def pieces_of(x):
    head = x.astype(jnp.bfloat16).astype(jnp.float32)
    rest = (x - head).astype(jnp.bfloat16).astype(jnp.float32)
    return head, rest, x - head - rest


def carried_in(block, first):
    lane = lanes_of(block.shape[0])
    return jnp.sum(jnp.where((lane >= first) & (lane < first + 3), block, 0.0), axis=1, keepdims=True)


def spread_rows(rows, core, sources, level, mains, inner, edge):
    levels = sources[0].shape[0] // rows
    half = rows // 2
    at = pl.ds(level, levels)
    k = 0
    for src, main, width in zip(sources, mains, (HALO, 1, HALO)):
        for j in range(half):
            main[at, j * B : (j + 1) * B] = src[pl.ds(core * half + j, levels, stride=rows), :]
        for j in range(width):
            near = jnp.where(core == 0, half + j, half - width + j)
            far = jnp.where(core == 0, j, rows - width + j)
            lanes = slice(k * B, (k + 1) * B)
            inner[at, lanes] = src[pl.ds(near, levels, stride=rows), :]
            edge[at, lanes] = src[pl.ds(far, levels, stride=rows), :].astype(edge.dtype)
            k += 1


def arrange_own(
    rows, lookup, weight, mixing, diffusion, radiance, inc, u, v,
    main_i, main_u, main_v, inner, edge, par, places, weights,
    lookup_at, weight_at, mixing_at, diffusion_at, radiance_at, inc_at, u_at, v_at, arrived,
):
    core = lax.axis_index("lev")
    here = (lookup_at, weight_at, mixing_at, diffusion_at, radiance_at, inc_at, u_at, v_at)
    copies = [
        pltpu.make_async_copy(src, dst, arrived.at[i])
        for i, (src, dst) in enumerate(
            zip((lookup, weight, mixing, diffusion, radiance, inc, u, v), here)
        )
    ]
    for copy in copies:
        copy.start()
    for copy in copies[:5]:
        copy.wait()
    places[...] = lookup_at[...] - core * main_i.shape[1]
    part, levels = mixing.shape
    weights[...] = jnp.broadcast_to(as_column(weight_at[...]), weights.shape)
    par[:, :B] = jnp.broadcast_to(as_column(diffusion_at[...]), (part, B))
    par[:, :levels] = mixing_at[...]
    par[:, B:] = radiance_at[...].astype(jnp.float32)
    for copy in copies[5:]:
        copy.wait()
    level = pl.multiple_of(core * part, 8)
    spread_rows(rows, core, (inc_at, u_at, v_at), level, (main_i, main_u, main_v), inner, edge)


def arrange_other(
    rows, inc, u, v, main_i0, main_u0, main_v0, inner0, edge0, main_i, main_u, main_v, inner, edge
):
    core = lax.axis_index("lev")
    level = pl.multiple_of((1 - core) * (inc.shape[0] // rows), 8)
    spread_rows(rows, core, (inc, u, v), level, (main_i, main_u, main_v), inner, edge)


def one_hot(counts, after, places, hot):
    columns = hot.shape[0]
    slots, width = places.shape
    index = lax.broadcasted_iota(jnp.int32, (columns, width), 0)
    for s in range(slots):
        place = jnp.where(s < counts[0, 0], places[s : s + 1, :], -1)
        hot[:, s * width : (s + 1) * width] = jnp.where(index == place, 1.0, 0.0).astype(jnp.bfloat16)


def by_column(after, hot, observed, out, live, stacked):
    steps, slots, channels, width = observed.shape
    for s in range(slots):
        for t in range(steps):
            stacked[t * channels : (t + 1) * channels, s * width : (s + 1) * width] = observed[t, s]
    tail = stacked.shape[0] - steps * channels
    stacked[steps * channels :, :] = jnp.ones((tail, slots * width), jnp.bfloat16)
    moved = lax.dot_general(
        stacked[...], hot[...], (((1,), (1,)), ((), ())), preferred_element_type=jnp.float32
    )
    out[...] = moved[: steps * channels].astype(jnp.bfloat16)
    live[...] = moved[steps * channels : steps * channels + 8]


def flags():
    core, lat = lax.axis_index("lev"), lax.axis_index("lat")
    first = (core == 1) | (lat > 0)
    final = (core == 0) | (lat < lax.axis_size("lat") - 1)
    return core, first, final


def fill_halo(win, near, far, low, width):
    count = win.shape[1] // B
    win[:, (HALO - width) * B : HALO * B] = jnp.where(low, far, near)
    win[:, (count - HALO) * B : (count - HALO + width) * B] = jnp.where(low, near, far)


def windows(main_i, main_u, main_v, inner, edge, after, win_i, win_u, win_v, packed):
    low = lax.axis_index("lev") == 0
    count = win_i.shape[1] // B
    k = 0
    for main, win, width, scale in ((main_i, win_i, HALO, 1.0), (main_u, win_u, 1, 0.5), (main_v, win_v, HALO, 0.5)):
        win[:, HALO * B : (count - HALO) * B] = scale * main[...]
        span = slice(k * B, (k + width) * B)
        fill_halo(win, scale * inner[:, span], scale * edge[:, span].astype(jnp.float32), low, width)
        k += width
    packed[...] = pack_edges(
        [functools.partial(block, win) for win in (win_i, win_u, win_v)], count - 2
    ).astype(packed.dtype)


def smooth(x, north, south, east, west, diff, u, v):
    return x + diff * ((north + south) + (east + west) - 4.0 * x) - u * (east - west) - v * (north - south)


def forward(
    win_i, win_u, win_v, west, own, east, own_par, other_par, observed, live, weights,
    f1, f2, edge, inner, cost, par, stack, plain, state,
):
    core, is_first, is_final = flags()
    part = own_par.shape[0]
    par[pl.ds(pl.multiple_of(core * part, 8), part), :] = own_par[...]
    par[pl.ds(pl.multiple_of((1 - core) * part, 8), part), :] = other_par[...]
    levels = par.shape[0]
    count = win_i.shape[1] // B
    rows = count - 2
    half = rows - 2
    diff = jnp.broadcast_to(par[:, levels : levels + 1], (levels, B))
    coupling = split_matrix(par[:, :B], levels)
    radiance = par[:, B:].astype(jnp.bfloat16)
    channels = radiance.shape[1]
    scale = weights[:, :1]
    clear_rest(stack, levels)
    sides = [side_block(west, own, east, f, rows) for f in range(3)]
    ends = both_ends(sides[0], sides[0])
    for q in range(rows):
        p = q + 1
        x, here = block(win_i, p), beyond(ends, q)
        s = smooth(
            x, block(win_i, p + 1), block(win_i, p - 1), from_east(x, here), from_west(x, here),
            diff, block(win_u, p), block(win_v, p),
        )
        plain[:, q * B : (q + 1) * B] = s
        put(stack, q, s)
    x = sides[0]
    s = smooth(x, roll(x, -GROUP), roll(x, GROUP), roll(x, -1), roll(x, 1), diff, sides[1], sides[2])
    plain[:, rows * B :] = s
    put(stack, rows, s)
    state[...] = plain[...] + jnp.dot(coupling, stack[...], preferred_element_type=jnp.float32)
    first, final = (rows - 1) * B, rows * B
    state[:, :B] = jnp.where(is_first, state[:, :B], 0.0)
    state[:, first:final] = jnp.where(is_final, state[:, first:final], 0.0)

    def observe(profile, t, out):
        evolved = lax.dot_general(
            radiance, profile, (((0,), (0,)), ((), ())), preferred_element_type=jnp.float32
        )
        departure = evolved - observed[t * channels : (t + 1) * channels, :].astype(jnp.float32)
        misfit = live[0:1, :] * departure
        scaled = scale * misfit
        back = jnp.dot(radiance, scaled.astype(jnp.bfloat16), preferred_element_type=jnp.float32)
        out[...] = back.astype(jnp.bfloat16)
        return jnp.sum(misfit * scaled, keepdims=True)

    total = observe(state[:, B : (half + 1) * B].astype(jnp.bfloat16), 0, f1)
    ends = both_ends(state[:, rows * B :], state[:, rows * B :])
    for q in range(1, rows - 1):
        x, here = block(state, q), beyond(ends, q)
        s = smooth(
            x, block(state, q + 1), block(state, q - 1), from_east(x, here), from_west(x, here),
            diff, block(win_u, q + 1), block(win_v, q + 1),
        )
        plain[:, (q - 1) * B : q * B] = s
        put(stack, q - 1, s)
    end = plain[:, : half * B] + jnp.dot(coupling, stack[:, : half * B], preferred_element_type=jnp.float32)
    total = total + observe(end.astype(jnp.bfloat16), 1, f2)
    whole = win_i[:, HALO * B : (count - HALO) * B]
    total = 0.5 * (total + jnp.sum(whole * whole, keepdims=True))
    cost[...] = jnp.broadcast_to(total, cost.shape)
    low = core == 0
    k = 0
    for f, width in ((f2, HALO), (f1, 1)):
        head, tail = f[:, : width * B].astype(jnp.float32), f[:, (half - width) * B :].astype(jnp.float32)
        edge[:levels, k * B : (k + width) * B] = jnp.where(low, head, tail).astype(jnp.bfloat16)
        inner[:, k * B : (k + width) * B] = jnp.where(low, tail, head).astype(jnp.bfloat16)
        k += width
    tail = edge.shape[0] - levels
    lane = lanes_of(tail)
    carried = jnp.zeros((tail, B), jnp.float32)
    for i, piece in enumerate(pieces_of(total)):
        carried = jnp.where(lane == i, piece, carried)
    edge[levels:, :B] = carried.astype(jnp.bfloat16)
    edge[levels:, B:] = jnp.zeros((tail, edge.shape[1] - B), jnp.bfloat16)


def forcing_windows(f1, f2, edge, inner, cost, win_1, win_2, packed, total):
    core, is_first, is_final = flags()
    low = core == 0
    inside = is_first & is_final
    levels = f1.shape[0]
    count = win_1.shape[1] // B
    k = 0
    for f, win, width in ((f2, win_2, HALO), (f1, win_1, 1)):
        win[:, HALO * B : (count - HALO) * B] = f[...].astype(jnp.float32)
        span = slice(k * B, (k + width) * B)
        far = jnp.where(inside, edge[:levels, span].astype(jnp.float32), 0.0)
        fill_halo(win, inner[:, span].astype(jnp.float32), far, low, width)
        k += width
    both = pack_edges([functools.partial(block, win) for win in (win_2, win_1)], count - 2)
    here = cost[...] + carried_in(edge[levels:, :B].astype(jnp.float32), 0)[: cost.shape[0]]
    total[...] = here
    lane = lanes_of(both.shape[0])
    for i, piece in enumerate(pieces_of(here[0:1, :])):
        both = jnp.where(lane == B - 3 + i, piece, both)
    packed[...] = both.astype(packed.dtype)


def add_sides(cost, one, two, *refs):
    *more, total = refs
    west, east = by_side(one, two)
    here = cost[...] + carried_in(west, B - 3)[: cost.shape[0]]
    if more:
        here = here + carried_in(east, B - 3)[: cost.shape[0]]
    for other in more:
        here = here + other[...]
    total[...] = here


def backward(
    win_1, win_2, fwest, fown, feast, win_i, win_u, win_v, west, own, east, par, after,
    kept, sent, stack, coupled, square,
):
    core, is_first, is_final = flags()
    levels = par.shape[0]
    count = win_i.shape[1] // B
    rows = count - 2
    half = rows - 2
    diff = jnp.broadcast_to(par[:, levels : levels + 1], (levels, B))
    middle = 1.0 - 4.0 * diff
    square[...] = jnp.zeros(square.shape, jnp.float32)
    square[:levels, :] = jnp.where(lanes_of(levels) < levels, par[:, :B], 0.0)
    coupling = split_matrix(jnp.transpose(square[...])[:levels], levels)
    clear_rest(stack, levels)
    f_sides = [side_block(fwest, fown, feast, f, rows) for f in range(2)]
    sides = [side_block(west, own, east, f, rows) for f in range(3)]
    for p in range(count):
        x = block(win_2, p)
        coupled[:, p * B : (p + 1) * B] = x
        put(stack, p, x)
    coupled[:, count * B :] = f_sides[0]
    put(stack, count, f_sides[0])
    coupled[...] = coupled[...] + jnp.dot(coupling, stack[...], preferred_element_type=jnp.float32)

    def ends_of(side):
        return both_ends((diff + sides[1]) * side, (diff - sides[1]) * side)

    def spread(p, q, ends):
        x, here = block(coupled, p), beyond(ends, q)
        north = (diff + block(win_v, q + 2)) * block(coupled, p + 1)
        south = (diff - block(win_v, q)) * block(coupled, p - 1)
        u = block(win_u, q + 1)
        return (
            middle * x + (north + south) + (from_east((diff + u) * x, here) + from_west((diff - u) * x, here))
        )

    side = coupled[:, count * B :]
    after = []
    side_v, side_u = sides[2], sides[1]
    result = (
        middle * side
        + roll((diff + side_v) * side, -GROUP)
        + roll((diff - side_v) * side, GROUP)
        + roll((diff + side_u) * side, -1)
        + roll((diff - side_u) * side, 1)
        + f_sides[1]
    )
    ends = ends_of(side)
    for q in range(rows):
        after.append(spread(q + 1, q, ends) + block(win_1, q + 1))
    after[0] = jnp.where(is_first, after[0], 0.0)
    after[-1] = jnp.where(is_final, after[-1], 0.0)
    for q in range(rows):
        coupled[:, (q + 1) * B : (q + 2) * B] = after[q]
        put(stack, q, after[q])
    coupled[:, count * B :] = result
    put(stack, rows, result)
    mixed = jnp.dot(coupling, stack[:, : (rows + 1) * B], preferred_element_type=jnp.float32)
    coupled[:, B : (rows + 1) * B] = coupled[:, B : (rows + 1) * B] + mixed[:, : rows * B]
    ends = ends_of(coupled[:, count * B :] + mixed[:, rows * B :])
    low = core == 0
    part = levels // 2
    for j in range(half):
        value = block(win_i, j + HALO) + spread(j + HALO, j + 1, ends)
        kept[pl.ds(j, part, stride=half), :] = jnp.where(low, value[:part], value[part:])
        sent[pl.ds(j, part, stride=half), :] = jnp.where(low, value[part:], value[:part])


def write_half(kept, gradient, done):
    half = kept.shape[1]
    at = pl.multiple_of(lax.axis_index("lev") * half, 8)
    copy = pltpu.make_async_copy(kept, gradient.at[:, pl.ds(at, half), :], done)
    copy.start()
    copy.wait()


def finish(cells, got, cost, cost_2, begun, gradient, value, value_at, done):
    half = got.shape[1]
    at = pl.multiple_of((1 - lax.axis_index("lev")) * half, 8)
    copy = pltpu.make_async_copy(got, gradient.at[:, pl.ds(at, half), :], done.at[0])
    copy.start()
    value_at[0, 0] = jnp.max(cost[0:1, :] + cost_2[0:1, :]) / cells
    last = pltpu.make_async_copy(value_at, value, done.at[1])
    last.start()
    copy.wait()
    last.wait()


def call(kernel, outs, scratch=(), aliases=None, from_hbm=False, smem=0, spaces=None, results=None, flops=10**9):
    spaces, results = dict(spaces or {}), dict(results or {})
    spaces.update({i: pltpu.SMEM for i in range(smem)})

    def run(*operands):
        if from_hbm:
            operands = [pltpu.with_memory_space_constraint(x, pltpu.HBM) for x in operands]
        usual = pltpu.HBM if from_hbm else pltpu.VMEM
        return pl.pallas_call(
            kernel,
            out_shape=[jax.ShapeDtypeStruct(shape, dtype) for shape, dtype in outs],
            in_specs=[pl.BlockSpec(memory_space=spaces.get(i, usual)) for i in range(len(operands))],
            out_specs=[pl.BlockSpec(memory_space=results.get(i, pltpu.VMEM)) for i in range(len(outs))],
            scratch_shapes=[shape if dtype is None else pltpu.VMEM(shape, dtype) for shape, dtype in scratch],
            input_output_aliases=aliases or {},
            cost_estimate=pl.CostEstimate(flops=flops, bytes_accessed=0, transcendentals=0),
            compiler_params=pltpu.CompilerParams(vmem_limit_bytes=24 * 2**20),
        )(*operands)

    return run


def beside(x):
    count = lax.axis_size("lon")
    got = []
    for first in (1, 0):
        pairs = [((2 * i + first) % count, (2 * i + first + 1) % count) for i in range(count // 2)]
        got.append(lax.ppermute(x, "lon", pairs + [(b, a) for a, b in pairs] if count > 2 else [(0, 1), (1, 0)]))
    return got


def ring(x, axis, shift):
    count = lax.axis_size(axis)
    return lax.ppermute(x, axis, [(i, (i + shift) % count) for i in range(count)])


def body(
    increment, wind_u, wind_v, diffusion, mixing, jacobian, obs_weight, innovation, counts, column_lookup
):
    part, rows, width = increment.shape
    levels = mixing.shape[1]
    steps, channels = innovation.shape[0], innovation.shape[-2]
    slots = innovation.shape[3]
    assert width == B and steps == HALO and levels == 2 * part
    half = rows // 2
    count = half + 2 * HALO
    columns = half * B
    f32, bf16 = jnp.float32, jnp.bfloat16
    tiles, along = lax.axis_size("lat"), lax.axis_size("lon")
    pairs = [(2 * i + 1, (2 * i + 2) % (2 * tiles)) for i in range(tiles)]
    pairs = pairs + [(b, a) for a, b in pairs]
    inside = [(a, b) for a, b in pairs if abs(a - b) == 1]

    def swap(x):
        return lax.ppermute(x, "lev", [(0, 1), (1, 0)])

    def across(x, which):
        return lax.ppermute(x, ("lat", "lev"), which)

    fields = [x.reshape(part * rows, B) for x in (increment, wind_u, wind_v)]
    others = [swap(x) for x in fields]
    halo = 2 * HALO + 1
    main = ((levels, columns), f32)
    groups = [main] * 3 + [((levels, halo * B), f32), ((levels, halo * B), bf16)]
    win = ((levels, count * B), f32)
    packed = ((levels, B), bf16)
    field = ((part * rows, B), f32)
    scalar = ((8, B), f32)
    waits = pltpu.SemaphoreType.DMA
    *sorted_rows, own_par, places, weights = call(
        functools.partial(arrange_own, rows),
        groups + [((part, 2 * B), f32), ((slots, B), jnp.int32), ((channels, B), f32)],
        [((slots, B), jnp.int32), ((1, channels), f32)]
        + [((part, levels), f32), ((1, part), f32), ((part, channels), bf16)]
        + [field] * 3
        + [(waits((8,)), None)],
        from_hbm=True,
    )(
        column_lookup.reshape(slots, B), obs_weight.reshape(1, -1), mixing, diffusion.reshape(1, -1),
        jacobian.T, *fields,
    )
    *mains, inner, edge = call(
        functools.partial(arrange_other, rows), groups,
        aliases={3 + i: i for i in range(5)},
    )(*others, *sorted_rows)
    edge = across(edge, inside)
    other_par = swap(own_par)
    (hot,) = call(one_hot, [((columns, slots * B), bf16)], smem=1)(counts, inner, places)
    win_i, win_u, win_v, own = call(windows, [win] * 3 + [packed])(*mains, inner, edge, hot)
    observed, live = call(
        by_column,
        [((steps * channels, columns), bf16), ((8, columns), f32)],
        [((steps * channels + 16, slots * B), bf16)],
    )(own, hot, innovation.reshape(steps, slots, channels, B))
    west, east = beside(own)
    forcing = ((levels, columns), bf16)
    depth = max(-(-3 * levels // 16) * 16, 2 * B)
    f1, f2, f_edge, f_inner, cost, par = call(
        forward,
        [forcing] * 2
        + [((levels + 16, (HALO + 1) * B), bf16), ((levels, (HALO + 1) * B), bf16)]
        + [scalar, ((levels, 2 * B), f32)],
        [((depth, (count - 1) * B), bf16), ((levels, (count - 1) * B), f32), ((levels, (count - 1) * B), f32)],
    )(win_i, win_u, win_v, west, own, east, own_par, other_par, observed, live, weights)
    few_points = along == 4
    f_edge, f_inner = across(f_edge, pairs), swap(f_inner)
    far_cost = ring(cost, "lon", 2) if few_points else None
    win_1, win_2, f_own, total = call(forcing_windows, [win] * 2 + [packed, scalar])(f1, f2, f_edge, f_inner, cost)
    f_west, f_east = beside(f_own)
    more = []
    if few_points:
        flip = [(i, i ^ 1) for i in range(tiles)]
        more = [far_cost, lax.ppermute(far_cost, "lat", flip)]
    (total,) = call(add_sides, [scalar], flops=10**7)(total, f_west, f_east, *more)
    more = ring(total, "lat", 2) if tiles > 2 else None
    kept, sent = call(
        backward,
        [((part * half, B), f32)] * 2,
        [((depth, (count + 1) * B), bf16), ((levels, (count + 1) * B), f32), ((B, B), f32)],
    )(win_1, win_2, f_west, f_own, f_east, win_i, win_u, win_v, west, own, east, par, total)
    if more is not None:
        total = total + more
    for axis, size, few in (("lat", tiles, False), ("lon", along, few_points)):
        shift = 4 if axis == "lat" else 2
        while shift < size and not few:
            total = total + ring(total, axis, shift)
            shift *= 2
    cells = increment.size * tiles * along * lax.axis_size("lev")
    got = swap(sent).reshape(part, half, B)
    total_2 = swap(total)
    (begun,) = call(
        write_half, [(increment.shape, f32)], [(waits(()), None)], results={0: pl.ANY}
    )(kept.reshape(part, half, B))
    gradient, value = call(
        functools.partial(finish, float(cells)),
        [(increment.shape, f32), ((1, 1), f32)],
        [(pltpu.SMEM((1, 1), f32), None), (waits((2,)), None)],
        spaces={3: pl.ANY},
        results={0: pl.ANY, 1: pl.ANY},
        aliases={3: 0},
    )(got, total, total_2, begun)
    return gradient, value.reshape(())


def solution(mesh):
    for axis in ("lat", "lon"):
        assert mesh.shape[axis] & (mesh.shape[axis] - 1) == 0 and mesh.shape[axis] > 1
    in_specs = (
        P("lev", "lat", "lon"),
        P("lev", "lat", "lon"),
        P("lev", "lat", "lon"),
        P("lev"),
        P("lev", None),
        P(None, "lev"),
        P(),
        P(None, "lat", "lon", None, None, None),
        P("lat", "lon"),
        P("lat", "lon", None),
    )
    out_specs = (P("lev", "lat", "lon"), P())

    return jax.shard_map(body, mesh=mesh, in_specs=in_specs, out_specs=out_specs, check_vma=False)
```

```python
import functools

import jax
import jax.numpy as jnp
from jax import lax
from jax.experimental import pallas as pl
from jax.experimental.pallas import tpu as pltpu
from jax.sharding import PartitionSpec as P


B = 128
HALO = 2
GROUP = 4


def roll(x, shift):
    shift %= B
    return x if shift == 0 else pltpu.roll(x, shift, 1)


def lanes_of(level_count):
    return lax.broadcasted_iota(jnp.int32, (level_count, B), 1)


def block(ref, p):
    return ref[:, p * B : (p + 1) * B]


def pack_edges(fields, rows, which, packed=None):
    for f, field in enumerate(fields):
        for q in which:
            rolled = roll(field(q + 1), (f * rows + q) * GROUP + 2)
            if packed is None:
                packed = jnp.zeros_like(rolled)
            packed = jnp.where(lanes_of(rolled.shape[0]) // GROUP == f * rows + q, rolled, packed)
    return packed


def by_side(one, two):
    even = lax.axis_index("lon") % 2 == 0
    one, two = one[...].astype(jnp.float32), two[...].astype(jnp.float32)
    return jnp.where(even, one, two), jnp.where(even, two, one)


def side_block(one, own, two, f, rows):
    west, east = by_side(one, two)
    own = own[...].astype(jnp.float32)
    return side_block_of(west, own, east, f, rows)


def side_block_of(west, own, east, f, rows):
    lane = lanes_of(own.shape[0])
    first = lane % GROUP < 2
    low, high = -f * rows * GROUP, B // 2 - f * rows * GROUP
    western = jnp.where(first, roll(west, low), roll(own, low))
    eastern = jnp.where(first, roll(own, high), roll(east, high))
    return jnp.where(lane < B // 2, western, eastern)


def both_ends(from_east, from_west):
    lane = lanes_of(from_east.shape[0])
    return jnp.where(lane % GROUP == 0, roll(from_east, -(B // 2 + 2)), from_west)


def beyond(ends, q):
    return roll(ends, B - 1 - q * GROUP)


def from_east(x, ends):
    return jnp.where(lanes_of(x.shape[0]) == B - 1, ends, roll(x, -1))


def from_west(x, ends):
    return jnp.where(lanes_of(x.shape[0]) == 0, ends, roll(x, 1))


def put(stack, p, x):
    levels = x.shape[0]
    head = x.astype(jnp.bfloat16)
    stack[0:levels, p * B : (p + 1) * B] = head
    stack[levels : 2 * levels, p * B : (p + 1) * B] = head
    stack[2 * levels : 3 * levels, p * B : (p + 1) * B] = (x - head.astype(jnp.float32)).astype(jnp.bfloat16)


def clear_rest(stack, levels):
    if stack.shape[0] > 3 * levels:
        stack[3 * levels :, :] = jnp.zeros((stack.shape[0] - 3 * levels, stack.shape[1]), stack.dtype)


def split_matrix(matrix, levels):
    lane = lanes_of(levels)
    matrix = jnp.where(lane < levels, matrix, 0.0)
    head = matrix.astype(jnp.bfloat16).astype(jnp.float32)
    rest = matrix - head
    over = B - levels
    low = jnp.where(lane < levels, head, roll(rest, levels))
    high = jnp.where(lane < levels - over, roll(rest, -over), roll(head, levels - over))
    high = jnp.where(lane < 2 * levels - over, high, 0.0)
    return jnp.concatenate([low, high], axis=1).astype(jnp.bfloat16)


def as_column(row):
    shape = (row.shape[1], row.shape[1])
    square = lax.broadcasted_iota(jnp.int32, shape, 0) == lax.broadcasted_iota(jnp.int32, shape, 1)
    return jnp.sum(jnp.where(square, row, 0.0), axis=1, keepdims=True)


def pieces_of(x):
    head = x.astype(jnp.bfloat16).astype(jnp.float32)
    rest = (x - head).astype(jnp.bfloat16).astype(jnp.float32)
    return head, rest, x - head - rest


def carried_in(block, first):
    lane = lanes_of(block.shape[0])
    return jnp.sum(jnp.where((lane >= first) & (lane < first + 3), block, 0.0), axis=1, keepdims=True)


def spread_rows(rows, core, sources, level, mains, inner, edge):
    levels = sources[0].shape[0] // rows
    half = rows // 2
    at = pl.ds(level, levels)
    k = 0
    for src, main, width in zip(sources, mains, (HALO, 1, HALO)):
        for j in range(half):
            main[at, j * B : (j + 1) * B] = src[pl.ds(core * half + j, levels, stride=rows), :]
        for j in range(width):
            near = jnp.where(core == 0, half + j, half - width + j)
            far = jnp.where(core == 0, j, rows - width + j)
            lanes = slice(k * B, (k + 1) * B)
            inner[at, lanes] = src[pl.ds(near, levels, stride=rows), :]
            edge[at, lanes] = src[pl.ds(far, levels, stride=rows), :].astype(edge.dtype)
            k += 1


def arrange_own(
    rows, lookup, weight, mixing, diffusion, radiance, inc, u, v,
    main_i, main_u, main_v, inner, edge, par, places, weights,
    lookup_at, weight_at, mixing_at, diffusion_at, radiance_at, inc_at, u_at, v_at, arrived,
):
    core = lax.axis_index("lev")
    here = (lookup_at, weight_at, mixing_at, diffusion_at, radiance_at, inc_at, u_at, v_at)
    copies = [
        pltpu.make_async_copy(src, dst, arrived.at[i])
        for i, (src, dst) in enumerate(
            zip((lookup, weight, mixing, diffusion, radiance, inc, u, v), here)
        )
    ]
    for copy in copies:
        copy.start()
    for copy in copies[:5]:
        copy.wait()
    places[...] = lookup_at[...] - core * main_i.shape[1]
    part, levels = mixing.shape
    weights[...] = jnp.broadcast_to(as_column(weight_at[...]), weights.shape)
    par[:, :B] = jnp.broadcast_to(as_column(diffusion_at[...]), (part, B))
    par[:, :levels] = mixing_at[...]
    par[:, B:] = radiance_at[...].astype(jnp.float32)
    for copy in copies[5:]:
        copy.wait()
    level = pl.multiple_of(core * part, 8)
    spread_rows(rows, core, (inc_at, u_at, v_at), level, (main_i, main_u, main_v), inner, edge)


def arrange_other(
    rows, inc, u, v, main_i0, main_u0, main_v0, inner0, edge0, main_i, main_u, main_v, inner, edge
):
    core = lax.axis_index("lev")
    level = pl.multiple_of((1 - core) * (inc.shape[0] // rows), 8)
    spread_rows(rows, core, (inc, u, v), level, (main_i, main_u, main_v), inner, edge)


def one_hot(counts, after, places, hot):
    columns = hot.shape[0]
    slots, width = places.shape
    index = lax.broadcasted_iota(jnp.int32, (columns, width), 0)
    for s in range(slots):
        place = jnp.where(s < counts[0, 0], places[s : s + 1, :], -1)
        hot[:, s * width : (s + 1) * width] = jnp.where(index == place, 1.0, 0.0).astype(jnp.bfloat16)


def by_column(after, hot, observed, out, live, stacked):
    steps, slots, channels, width = observed.shape
    for s in range(slots):
        for t in range(steps):
            stacked[t * channels : (t + 1) * channels, s * width : (s + 1) * width] = observed[t, s]
    tail = stacked.shape[0] - steps * channels
    stacked[steps * channels :, :] = jnp.ones((tail, slots * width), jnp.bfloat16)
    moved = lax.dot_general(
        stacked[...], hot[...], (((1,), (1,)), ((), ())), preferred_element_type=jnp.float32
    )
    out[...] = moved[: steps * channels].astype(jnp.bfloat16)
    live[...] = moved[steps * channels : steps * channels + 8]


def flags():
    core, lat = lax.axis_index("lev"), lax.axis_index("lat")
    first = (core == 1) | (lat > 0)
    final = (core == 0) | (lat < lax.axis_size("lat") - 1)
    return core, first, final


def fill_halo(win, near, far, low, width):
    count = win.shape[1] // B
    win[:, (HALO - width) * B : HALO * B] = jnp.where(low, far, near)
    win[:, (count - HALO) * B : (count - HALO + width) * B] = jnp.where(low, near, far)


def own_row(main, p):
    return block(main, p - HALO)


def pack_own(rows, main_i, main_u, main_v, packed):
    scaled = [functools.partial(own_row, main) for main in (main_i, main_u, main_v)]
    both = pack_edges(scaled, rows, range(1, rows - 1))
    field = lanes_of(both.shape[0]) // (GROUP * rows)
    packed[...] = (both * jnp.where(field == 0, 1.0, 0.5)).astype(packed.dtype)


def windows(main_i, main_u, main_v, inner, edge, after, own, win_i, win_u, win_v, packed):
    low = lax.axis_index("lev") == 0
    count = win_i.shape[1] // B
    k = 0
    for main, win, width, scale in ((main_i, win_i, HALO, 1.0), (main_u, win_u, 1, 0.5), (main_v, win_v, HALO, 0.5)):
        win[:, HALO * B : (count - HALO) * B] = scale * main[...]
        span = slice(k * B, (k + width) * B)
        fill_halo(win, scale * inner[:, span], scale * edge[:, span].astype(jnp.float32), low, width)
        k += width
    rows = count - 2
    packed[...] = pack_edges(
        [functools.partial(block, win) for win in (win_i, win_u, win_v)], rows, (0, rows - 1), own[...].astype(jnp.float32)
    ).astype(packed.dtype)


def smooth(x, north, south, east, west, diff, u, v):
    return x + diff * ((north + south) + (east + west) - 4.0 * x) - u * (east - west) - v * (north - south)


def forward(
    win_i, win_u, win_v, west, own, east, own_par, other_par, observed, live, weights,
    f1, f2, edge, inner, cost, par, stack, plain, state,
):
    core, is_first, is_final = flags()
    part = own_par.shape[0]
    par[pl.ds(pl.multiple_of(core * part, 8), part), :] = own_par[...]
    par[pl.ds(pl.multiple_of((1 - core) * part, 8), part), :] = other_par[...]
    levels = par.shape[0]
    count = win_i.shape[1] // B
    rows = count - 2
    half = rows - 2
    diff = jnp.broadcast_to(par[:, levels : levels + 1], (levels, B))
    coupling = split_matrix(par[:, :B], levels)
    radiance = par[:, B:].astype(jnp.bfloat16)
    channels = radiance.shape[1]
    scale = weights[:, :1]
    clear_rest(stack, levels)
    sides = [side_block(west, own, east, f, rows) for f in range(3)]
    ends = both_ends(sides[0], sides[0])
    for q in range(rows):
        p = q + 1
        x, here = block(win_i, p), beyond(ends, q)
        s = smooth(
            x, block(win_i, p + 1), block(win_i, p - 1), from_east(x, here), from_west(x, here),
            diff, block(win_u, p), block(win_v, p),
        )
        plain[:, q * B : (q + 1) * B] = s
        put(stack, q, s)
    x = sides[0]
    s = smooth(x, roll(x, -GROUP), roll(x, GROUP), roll(x, -1), roll(x, 1), diff, sides[1], sides[2])
    plain[:, rows * B :] = s
    put(stack, rows, s)
    state[...] = plain[...] + jnp.dot(coupling, stack[...], preferred_element_type=jnp.float32)
    first, final = (rows - 1) * B, rows * B
    state[:, :B] = jnp.where(is_first, state[:, :B], 0.0)
    state[:, first:final] = jnp.where(is_final, state[:, first:final], 0.0)

    def observe(profile, t, out):
        evolved = lax.dot_general(
            radiance, profile, (((0,), (0,)), ((), ())), preferred_element_type=jnp.float32
        )
        departure = evolved - observed[t * channels : (t + 1) * channels, :].astype(jnp.float32)
        misfit = live[0:1, :] * departure
        scaled = scale * misfit
        back = jnp.dot(radiance, scaled.astype(jnp.bfloat16), preferred_element_type=jnp.float32)
        out[...] = back.astype(jnp.bfloat16)
        return jnp.sum(misfit * scaled, keepdims=True)

    total = observe(state[:, B : (half + 1) * B].astype(jnp.bfloat16), 0, f1)
    ends = both_ends(state[:, rows * B :], state[:, rows * B :])
    for q in range(1, rows - 1):
        x, here = block(state, q), beyond(ends, q)
        s = smooth(
            x, block(state, q + 1), block(state, q - 1), from_east(x, here), from_west(x, here),
            diff, block(win_u, q + 1), block(win_v, q + 1),
        )
        plain[:, (q - 1) * B : q * B] = s
        put(stack, q - 1, s)
    end = plain[:, : half * B] + jnp.dot(coupling, stack[:, : half * B], preferred_element_type=jnp.float32)
    total = total + observe(end.astype(jnp.bfloat16), 1, f2)
    whole = win_i[:, HALO * B : (count - HALO) * B]
    total = 0.5 * (total + jnp.sum(whole * whole, keepdims=True))
    cost[...] = jnp.broadcast_to(total, cost.shape)
    low = core == 0
    k = 0
    for f, width in ((f2, HALO), (f1, 1)):
        head, tail = f[:, : width * B].astype(jnp.float32), f[:, (half - width) * B :].astype(jnp.float32)
        edge[:levels, k * B : (k + width) * B] = jnp.where(low, head, tail).astype(jnp.bfloat16)
        inner[:, k * B : (k + width) * B] = jnp.where(low, tail, head).astype(jnp.bfloat16)
        k += width
    tail = edge.shape[0] - levels
    lane = lanes_of(tail)
    carried = jnp.zeros((tail, B), jnp.float32)
    for i, piece in enumerate(pieces_of(total)):
        carried = jnp.where(lane == i, piece, carried)
    edge[levels:, :B] = carried.astype(jnp.bfloat16)
    edge[levels:, B:] = jnp.zeros((tail, edge.shape[1] - B), jnp.bfloat16)


def forcing_windows(f1, f2, edge, inner, cost, win_1, win_2, packed, total):
    core, is_first, is_final = flags()
    low = core == 0
    inside = is_first & is_final
    levels = f1.shape[0]
    count = win_1.shape[1] // B
    k = 0
    for f, win, width in ((f2, win_2, HALO), (f1, win_1, 1)):
        win[:, HALO * B : (count - HALO) * B] = f[...].astype(jnp.float32)
        span = slice(k * B, (k + width) * B)
        far = jnp.where(inside, edge[:levels, span].astype(jnp.float32), 0.0)
        fill_halo(win, inner[:, span].astype(jnp.float32), far, low, width)
        k += width
    both = pack_edges([functools.partial(block, win) for win in (win_2, win_1)], count - 2, range(count - 2))
    here = cost[...] + carried_in(edge[levels:, :B].astype(jnp.float32), 0)[: cost.shape[0]]
    total[...] = here
    lane = lanes_of(both.shape[0])
    for i, piece in enumerate(pieces_of(here[0:1, :])):
        both = jnp.where(lane == B - 3 + i, piece, both)
    packed[...] = both.astype(packed.dtype)


def add_sides(cost, one, two, *refs):
    *more, total = refs
    west, east = by_side(one, two)
    here = cost[...] + carried_in(west, B - 3)[: cost.shape[0]]
    if more:
        here = here + carried_in(east, B - 3)[: cost.shape[0]]
    for other in more:
        here = here + other[...]
    total[...] = here


def backward(
    win_1, win_2, fwest, fown, feast, win_i, win_u, win_v, west, own, east, par, after,
    kept, sent, stack, coupled, square,
):
    core, is_first, is_final = flags()
    levels = par.shape[0]
    count = win_i.shape[1] // B
    rows = count - 2
    half = rows - 2
    diff = jnp.broadcast_to(par[:, levels : levels + 1], (levels, B))
    middle = 1.0 - 4.0 * diff
    square[...] = jnp.zeros(square.shape, jnp.float32)
    square[:levels, :] = jnp.where(lanes_of(levels) < levels, par[:, :B], 0.0)
    coupling = split_matrix(jnp.transpose(square[...])[:levels], levels)
    clear_rest(stack, levels)
    f_sides = [side_block(fwest, fown, feast, f, rows) for f in range(2)]
    sides = [side_block(west, own, east, f, rows) for f in range(3)]
    for p in range(count):
        x = block(win_2, p)
        coupled[:, p * B : (p + 1) * B] = x
        put(stack, p, x)
    coupled[:, count * B :] = f_sides[0]
    put(stack, count, f_sides[0])
    coupled[...] = coupled[...] + jnp.dot(coupling, stack[...], preferred_element_type=jnp.float32)

    def ends_of(side):
        return both_ends((diff + sides[1]) * side, (diff - sides[1]) * side)

    def spread(p, q, ends):
        x, here = block(coupled, p), beyond(ends, q)
        north = (diff + block(win_v, q + 2)) * block(coupled, p + 1)
        south = (diff - block(win_v, q)) * block(coupled, p - 1)
        u = block(win_u, q + 1)
        return (
            middle * x + (north + south) + (from_east((diff + u) * x, here) + from_west((diff - u) * x, here))
        )

    side = coupled[:, count * B :]
    after = []
    side_v, side_u = sides[2], sides[1]
    result = (
        middle * side
        + roll((diff + side_v) * side, -GROUP)
        + roll((diff - side_v) * side, GROUP)
        + roll((diff + side_u) * side, -1)
        + roll((diff - side_u) * side, 1)
        + f_sides[1]
    )
    ends = ends_of(side)
    for q in range(rows):
        after.append(spread(q + 1, q, ends) + block(win_1, q + 1))
    after[0] = jnp.where(is_first, after[0], 0.0)
    after[-1] = jnp.where(is_final, after[-1], 0.0)
    for q in range(rows):
        coupled[:, (q + 1) * B : (q + 2) * B] = after[q]
        put(stack, q, after[q])
    coupled[:, count * B :] = result
    put(stack, rows, result)
    mixed = jnp.dot(coupling, stack[:, : (rows + 1) * B], preferred_element_type=jnp.float32)
    coupled[:, B : (rows + 1) * B] = coupled[:, B : (rows + 1) * B] + mixed[:, : rows * B]
    ends = ends_of(coupled[:, count * B :] + mixed[:, rows * B :])
    low = core == 0
    part = levels // 2
    for j in range(half):
        value = block(win_i, j + HALO) + spread(j + HALO, j + 1, ends)
        kept[pl.ds(j, part, stride=half), :] = jnp.where(low, value[:part], value[part:])
        sent[pl.ds(j, part, stride=half), :] = jnp.where(low, value[part:], value[:part])


def write_half(kept, gradient, done):
    half = kept.shape[1]
    at = pl.multiple_of(lax.axis_index("lev") * half, 8)
    copy = pltpu.make_async_copy(kept, gradient.at[:, pl.ds(at, half), :], done)
    copy.start()
    copy.wait()


def finish(cells, got, cost, cost_2, begun, gradient, value, value_at, done):
    half = got.shape[1]
    at = pl.multiple_of((1 - lax.axis_index("lev")) * half, 8)
    copy = pltpu.make_async_copy(got, gradient.at[:, pl.ds(at, half), :], done.at[0])
    copy.start()
    value_at[0, 0] = jnp.max(cost[0:1, :] + cost_2[0:1, :]) / cells
    last = pltpu.make_async_copy(value_at, value, done.at[1])
    last.start()
    copy.wait()
    last.wait()


def call(kernel, outs, scratch=(), aliases=None, from_hbm=False, smem=0, spaces=None, results=None, flops=10**9):
    spaces, results = dict(spaces or {}), dict(results or {})
    spaces.update({i: pltpu.SMEM for i in range(smem)})

    def run(*operands):
        if from_hbm:
            operands = [pltpu.with_memory_space_constraint(x, pltpu.HBM) for x in operands]
        usual = pltpu.HBM if from_hbm else pltpu.VMEM
        return pl.pallas_call(
            kernel,
            out_shape=[jax.ShapeDtypeStruct(shape, dtype) for shape, dtype in outs],
            in_specs=[pl.BlockSpec(memory_space=spaces.get(i, usual)) for i in range(len(operands))],
            out_specs=[pl.BlockSpec(memory_space=results.get(i, pltpu.VMEM)) for i in range(len(outs))],
            scratch_shapes=[shape if dtype is None else pltpu.VMEM(shape, dtype) for shape, dtype in scratch],
            input_output_aliases=aliases or {},
            cost_estimate=pl.CostEstimate(flops=flops, bytes_accessed=0, transcendentals=0),
            compiler_params=pltpu.CompilerParams(vmem_limit_bytes=24 * 2**20),
        )(*operands)

    return run


def beside(x):
    count = lax.axis_size("lon")
    got = []
    for first in (1, 0):
        pairs = [((2 * i + first) % count, (2 * i + first + 1) % count) for i in range(count // 2)]
        got.append(lax.ppermute(x, "lon", pairs + [(b, a) for a, b in pairs] if count > 2 else [(0, 1), (1, 0)]))
    return got


def ring(x, axis, shift):
    count = lax.axis_size(axis)
    return lax.ppermute(x, axis, [(i, (i + shift) % count) for i in range(count)])


def body(
    increment, wind_u, wind_v, diffusion, mixing, jacobian, obs_weight, innovation, counts, column_lookup
):
    part, rows, width = increment.shape
    levels = mixing.shape[1]
    steps, channels = innovation.shape[0], innovation.shape[-2]
    slots = innovation.shape[3]
    assert width == B and steps == HALO and levels == 2 * part
    half = rows // 2
    count = half + 2 * HALO
    columns = half * B
    f32, bf16 = jnp.float32, jnp.bfloat16
    tiles, along = lax.axis_size("lat"), lax.axis_size("lon")
    pairs = [(2 * i + 1, (2 * i + 2) % (2 * tiles)) for i in range(tiles)]
    pairs = pairs + [(b, a) for a, b in pairs]
    inside = [(a, b) for a, b in pairs if abs(a - b) == 1]

    def swap(x):
        return lax.ppermute(x, "lev", [(0, 1), (1, 0)])

    def across(x, which):
        return lax.ppermute(x, ("lat", "lev"), which)

    fields = [x.reshape(part * rows, B) for x in (increment, wind_u, wind_v)]
    others = [swap(x) for x in fields]
    halo = 2 * HALO + 1
    main = ((levels, columns), f32)
    groups = [main] * 3 + [((levels, halo * B), f32), ((levels, halo * B), bf16)]
    win = ((levels, count * B), f32)
    packed = ((levels, B), bf16)
    field = ((part * rows, B), f32)
    scalar = ((8, B), f32)
    waits = pltpu.SemaphoreType.DMA
    *sorted_rows, own_par, places, weights = call(
        functools.partial(arrange_own, rows),
        groups + [((part, 2 * B), f32), ((slots, B), jnp.int32), ((channels, B), f32)],
        [((slots, B), jnp.int32), ((1, channels), f32)]
        + [((part, levels), f32), ((1, part), f32), ((part, channels), bf16)]
        + [field] * 3
        + [(waits((8,)), None)],
        from_hbm=True,
    )(
        column_lookup.reshape(slots, B), obs_weight.reshape(1, -1), mixing, diffusion.reshape(1, -1),
        jacobian.T, *fields,
    )
    *mains, inner, edge = call(
        functools.partial(arrange_other, rows), groups,
        aliases={3 + i: i for i in range(5)},
    )(*others, *sorted_rows)
    edge = across(edge, inside)
    (own,) = call(functools.partial(pack_own, count - 2), [packed])(*mains)
    other_par = swap(own_par)
    (hot,) = call(one_hot, [((columns, slots * B), bf16)], smem=1)(counts, inner, places)
    win_i, win_u, win_v, own = call(windows, [win] * 3 + [packed])(*mains, inner, edge, hot, own)
    observed, live = call(
        by_column,
        [((steps * channels, columns), bf16), ((8, columns), f32)],
        [((steps * channels + 16, slots * B), bf16)],
    )(own, hot, innovation.reshape(steps, slots, channels, B))
    west, east = beside(own)
    forcing = ((levels, columns), bf16)
    depth = max(-(-3 * levels // 16) * 16, 2 * B)
    f1, f2, f_edge, f_inner, cost, par = call(
        forward,
        [forcing] * 2
        + [((levels + 16, (HALO + 1) * B), bf16), ((levels, (HALO + 1) * B), bf16)]
        + [scalar, ((levels, 2 * B), f32)],
        [((depth, (count - 1) * B), bf16), ((levels, (count - 1) * B), f32), ((levels, (count - 1) * B), f32)],
    )(win_i, win_u, win_v, west, own, east, own_par, other_par, observed, live, weights)
    few_points = along == 4
    f_edge, f_inner = across(f_edge, pairs), swap(f_inner)
    far_cost = ring(cost, "lon", 2) if few_points else None
    win_1, win_2, f_own, total = call(forcing_windows, [win] * 2 + [packed, scalar])(f1, f2, f_edge, f_inner, cost)
    f_west, f_east = beside(f_own)
    more = []
    if few_points:
        flip = [(i, i ^ 1) for i in range(tiles)]
        more = [far_cost, lax.ppermute(far_cost, "lat", flip)]
    (total,) = call(add_sides, [scalar], flops=10**7)(total, f_west, f_east, *more)
    more = ring(total, "lat", 2) if tiles > 2 else None
    kept, sent = call(
        backward,
        [((part * half, B), f32)] * 2,
        [((depth, (count + 1) * B), bf16), ((levels, (count + 1) * B), f32), ((B, B), f32)],
    )(win_1, win_2, f_west, f_own, f_east, win_i, win_u, win_v, west, own, east, par, total)
    if more is not None:
        total = total + more
    for axis, size, few in (("lat", tiles, False), ("lon", along, few_points)):
        shift = 4 if axis == "lat" else 2
        while shift < size and not few:
            total = total + ring(total, axis, shift)
            shift *= 2
    cells = increment.size * tiles * along * lax.axis_size("lev")
    got = swap(sent).reshape(part, half, B)
    total_2 = swap(total)
    (begun,) = call(
        write_half, [(increment.shape, f32)], [(waits(()), None)], results={0: pl.ANY}
    )(kept.reshape(part, half, B))
    gradient, value = call(
        functools.partial(finish, float(cells)),
        [(increment.shape, f32), ((1, 1), f32)],
        [(pltpu.SMEM((1, 1), f32), None), (waits((2,)), None)],
        spaces={3: pl.ANY},
        results={0: pl.ANY, 1: pl.ANY},
        aliases={3: 0},
    )(got, total, total_2, begun)
    return gradient, value.reshape(())


def solution(mesh):
    for axis in ("lat", "lon"):
        assert mesh.shape[axis] & (mesh.shape[axis] - 1) == 0 and mesh.shape[axis] > 1
    in_specs = (
        P("lev", "lat", "lon"),
        P("lev", "lat", "lon"),
        P("lev", "lat", "lon"),
        P("lev"),
        P("lev", None),
        P(None, "lev"),
        P(),
        P(None, "lat", "lon", None, None, None),
        P("lat", "lon"),
        P("lat", "lon", None),
    )
    out_specs = (P("lev", "lat", "lon"), P())

    return jax.shard_map(body, mesh=mesh, in_specs=in_specs, out_specs=out_specs, check_vma=False)
```
